8 devices in a mesh: dp: 1 (over z), tp: 8 (over y, x, core).
Axes of the slice: x: 2, y: 2, z: 1, core: 2. Of those that a mesh axis runs over, the one named last changes fastest.
Arguments:
- hidden: bfloat16 [16, 1536], P('dp')
- final_gain: bfloat16 [1536], replicated
- embed_table: bfloat16 [151936, 1536], P(None, 'tp')
- targets: int32 [16], P('dp')
- temperature: float32 [], replicated
Outputs:
- output 1: float32 [16], P('dp')
- output 2: float32 [16], P('dp')
- output 3: bfloat16 [16, 151936], P('dp', 'tp')
All inputs are finite; a program needn't handle non-finite values.
Results may differ from the reference program's by a relative error of at most 0.001.
Values sent between devices are 32-bit elements.
A program may use at most 1 GiB of HBM per device.

```python
import jax
import jax.numpy as jnp
from jax import lax

TOKENS = 16
HIDDEN = 1536
VOCABULARY = 151936
NORM_EPS = 1e-6
ROW_BLOCK = min(TOKENS, 32)


def setup_inputs(seed: int = 0, part: int = 0) -> dict:
    shared_key, part_root = jax.random.split(jax.random.key(seed))
    part_key = jax.random.fold_in(part_root, part)
    gain_key, table_key, temp_key = jax.random.split(shared_key, 3)
    hidden_key, perm_key, offset_key = jax.random.split(part_key, 3)
    hidden = jax.random.normal(hidden_key, (TOKENS, HIDDEN), jnp.float32).astype(jnp.bfloat16)
    final_gain = jax.random.uniform(gain_key, (HIDDEN,), jnp.float32, 0.5, 1.5).astype(jnp.bfloat16)
    embed_table = (jax.random.normal(table_key, (VOCABULARY, HIDDEN), jnp.float32) * (2.0 / HIDDEN ** 0.5)).astype(jnp.bfloat16)
    stride = VOCABULARY // TOKENS
    targets = (jax.random.permutation(perm_key, TOKENS).astype(jnp.int32) * stride
               + jax.random.randint(offset_key, (TOKENS,), 0, stride, jnp.int32))
    temperature = jax.random.uniform(temp_key, (), jnp.float32, 0.8, 1.25)
    return {'hidden': hidden, 'final_gain': final_gain, 'embed_table': embed_table,
            'targets': targets, 'temperature': temperature}


def reference(hidden, final_gain, embed_table, targets, temperature):
    hidden_f32 = hidden.astype(jnp.float32)
    inv_rms = lax.rsqrt(jnp.mean(hidden_f32 * hidden_f32, axis=-1, keepdims=True) + NORM_EPS)
    normed = (hidden_f32 * inv_rms * final_gain.astype(jnp.float32)).astype(jnp.bfloat16)
    num_blocks = TOKENS // ROW_BLOCK
    normed_blocks = normed.reshape(num_blocks, ROW_BLOCK, HIDDEN)
    target_blocks = targets.reshape(num_blocks, ROW_BLOCK)

    def score_block(block_pair):
        normed_rows, target_ids = block_pair
        logits = jnp.dot(normed_rows, embed_table.T, preferred_element_type=jnp.float32) / temperature
        row_max = jnp.max(logits, axis=-1, keepdims=True)
        log_norm = row_max[:, 0] + jnp.log(jnp.sum(jnp.exp(logits - row_max), axis=-1))
        target_logit = jnp.take_along_axis(logits, target_ids[:, None], axis=1)[:, 0]
        token_probs = jnp.exp(logits - log_norm[:, None]).astype(jnp.bfloat16)
        return log_norm, target_logit - log_norm, token_probs

    log_norm, target_logprob, token_probs = lax.map(score_block, (normed_blocks, target_blocks))
    return (log_norm.reshape(TOKENS), target_logprob.reshape(TOKENS),
            token_probs.reshape(TOKENS, VOCABULARY))
```

```python
import jax
import jax.numpy as jnp
from jax import lax
from jax.experimental import pallas as pl
from jax.experimental.pallas import tpu as pltpu
from jax.sharding import PartitionSpec as P

NORM_EPS = 1e-6
LANES = 128
LANE_CHUNKS = 5
DEPTH = 4
NEG = -3.0e38
MESH = pl.DeviceIdType.MESH


def _kernel(shape, hid_hbm, gain_hbm, table_hbm, tgt_hbm, temp_hbm, logits_ref, stats_ref,
            hid, gain, tgt, temp, normed, tbuf, psend, prec, own, r1, r2, mine, every,
            in_sem, tsem, d2d_ssem, d2d_rsem, s1_ssem, s1_rsem, s2_ssem, s2_rsem, st_ssem, st_rsem):
    vocab, rows_per, tokens, width, tiles, chunk = shape
    half_tiles = tiles // 2
    nl = LANE_CHUNKS
    steps = 4 * nl
    me = lax.axis_index('tp')
    core, mx, my = me % 2, (me // 2) % 2, me // 4
    partner = me + 1 - 2 * core
    xn = me + 2 - 4 * mx
    yn = me + 4 - 8 * my
    first = (xn, yn)
    second = (yn, xn)

    def region_tile(d):
        return (d * rows_per) // LANES - d // 7

    def table_copy(i, q):
        p, j = i // nl, i % nl
        lane = q % 2
        a, b = 1 - p // 2, 1 - p % 2
        fx, fy = (a, b) if lane == 0 else (b, a)
        k = 1 - core if q < 2 else core
        d = (my + fy * (1 - 2 * my)) * 4 + (mx + fx * (1 - 2 * mx)) * 2 + k
        tile = region_tile(d) + lane * half_tiles + j * (chunk // LANES)
        col = pl.multiple_of(tile * LANES, LANES)
        slot = (i % DEPTH) * 4 + q
        return pltpu.make_async_copy(table_hbm.at[:, pl.ds(col, chunk)], tbuf.at[slot], tsem.at[slot])

    for i in range(DEPTH):
        for q in range(4):
            if i == 0 and q == 2:
                pltpu.make_async_copy(hid_hbm, hid, in_sem.at[0]).start()
                pltpu.make_async_copy(gain_hbm, gain, in_sem.at[1]).start()
            table_copy(i, q).start()
    pltpu.make_async_copy(tgt_hbm, tgt, in_sem.at[2]).start()
    pltpu.make_async_copy(temp_hbm, temp, in_sem.at[3]).start()

    barrier = pltpu.get_barrier_semaphore()
    for r in range(1, 8):
        pl.semaphore_signal(barrier, inc=1, device_id={'tp': (me + r) % 8}, device_id_type=MESH)

    pltpu.make_async_copy(hid_hbm, hid, in_sem.at[0]).wait()
    pltpu.make_async_copy(gain_hbm, gain, in_sem.at[1]).wait()
    h = hid[...].astype(jnp.float32)
    inv_rms = lax.rsqrt(jnp.mean(h * h, axis=-1, keepdims=True) + NORM_EPS)
    col0 = pl.multiple_of(((me * 3) // 2) * LANES, LANES)
    hc = hid[:, pl.ds(col0, 2 * LANES)].astype(jnp.float32)
    gc = gain[:, pl.ds(col0, 2 * LANES)].astype(jnp.float32)
    u = hc * inv_rms * gc
    u = jnp.where(core == 0, u[:, :width], u[:, 2 * LANES - width:])
    normed[...] = u.astype(jnp.bfloat16)

    pl.semaphore_wait(barrier, 7)

    def d2d(s):
        return pltpu.make_async_remote_copy(
            src_ref=psend.at[s], dst_ref=prec.at[s], send_sem=d2d_ssem.at[s], recv_sem=d2d_rsem.at[s],
            device_id={'tp': partner}, device_id_type=MESH)

    def stage1(lane, i):
        s = i * 2 + lane
        return pltpu.make_async_remote_copy(
            src_ref=own.at[s], dst_ref=r1.at[s], send_sem=s1_ssem.at[s], recv_sem=s1_rsem.at[s],
            device_id={'tp': first[lane]}, device_id_type=MESH)

    def stage2(lane, j):
        s = j * 2 + lane
        return pltpu.make_async_remote_copy(
            src_ref=own.at[4 * nl + s], dst_ref=r2.at[s], send_sem=s2_ssem.at[s], recv_sem=s2_rsem.at[s],
            device_id={'tp': second[lane]}, device_id_type=MESH)

    def compute(i, prefetch):
        for q in range(4):
            s = i * 2 + q % 2
            slot = (i % DEPTH) * 4 + q
            table_copy(i, q).wait()
            out = psend if q < 2 else own
            out[s] = jnp.dot(normed[...], tbuf[slot], preferred_element_type=jnp.float32)
            if q < 2:
                d2d(s).start()
            if prefetch:
                table_copy(i + DEPTH, q).start()

    def gather_pair(i, send):
        for lane in range(2):
            s = i * 2 + lane
            d2d(s).wait_recv()
            own[s] = own[s] + prec[s]
            if send:
                stage1(lane, i).start()

    compute(0, True)

    def loop_send(i, carry):
        compute(i, True)
        gather_pair(i - 1, True)
        return carry

    def loop_keep(i, carry):
        compute(i, True)
        gather_pair(i - 1, False)
        return carry

    def loop_last(i, carry):
        compute(i, False)
        gather_pair(i - 1, False)
        return carry

    lax.fori_loop(1, 2 * nl + 1, loop_send, 0)
    lax.fori_loop(2 * nl + 1, steps - DEPTH, loop_keep, 0)
    lax.fori_loop(steps - DEPTH, steps, loop_last, 0)
    gather_pair(steps - 1, False)

    def forward(j, carry):
        for lane in range(2):
            stage1(lane, j).wait_recv()
            s = (2 * nl + j) * 2 + lane
            own[s] = own[s] + r1[j * 2 + lane]
            stage2(lane, j).start()
        return carry

    lax.fori_loop(0, nl, forward, 0)

    pltpu.make_async_copy(tgt_hbm, tgt, in_sem.at[2]).wait()
    pltpu.make_async_copy(temp_hbm, temp, in_sem.at[3]).wait()
    temperature = temp[0]
    row = lax.broadcasted_iota(jnp.int32, (tokens, LANES), 0)
    lane_id = lax.broadcasted_iota(jnp.int32, (tokens, LANES), 1)
    target = jnp.zeros((tokens, LANES), jnp.int32)
    for t in range(tokens):
        target = jnp.where(row == t, tgt[t], target)
    lo = me * rows_per
    base = region_tile(me) * LANES

    def finish(j, carry):
        m, total, picked = carry
        for lane in range(2):
            stage1(lane, nl + j).wait_recv()
            stage2(lane, j).wait_recv()
            z = own[(3 * nl + j) * 2 + lane] + r1[(nl + j) * 2 + lane] + r2[j * 2 + lane]
            t = z / temperature
            off = pl.multiple_of((lane * half_tiles + j * (chunk // LANES)) * LANES, LANES)
            logits_ref[:, pl.ds(off, chunk)] = t
            parts = []
            top = m
            for k in range(chunk // LANES):
                piece = t[:, k * LANES:(k + 1) * LANES]
                col = lane_id + (base + off + k * LANES)
                inside = (col >= lo) & (col < lo + rows_per)
                piece_in = jnp.where(inside, piece, NEG)
                picked = picked + jnp.where(inside & (col == target), piece, 0.0)
                parts.append(piece_in)
                top = jnp.maximum(top, piece_in)
            total = total * jnp.exp(m - top)
            for piece_in in parts:
                total = total + jnp.exp(piece_in - top)
            m = top
        return m, total, picked

    m, total, picked = lax.fori_loop(
        0, nl, finish,
        (jnp.full((tokens, LANES), NEG, jnp.float32), jnp.zeros((tokens, LANES), jnp.float32),
         jnp.zeros((tokens, LANES), jnp.float32)))
    m_row = jnp.max(m, axis=-1, keepdims=True)
    s_row = jnp.sum(total * jnp.exp(m - m_row), axis=-1, keepdims=True)
    p_row = jnp.sum(picked, axis=-1, keepdims=True)
    packed = jnp.where(lane_id == 0, m_row, jnp.where(lane_id == 1, s_row, p_row))
    mine[...] = packed

    def share(peer, slot):
        return pltpu.make_async_remote_copy(
            src_ref=mine, dst_ref=every.at[slot], send_sem=st_ssem.at[peer], recv_sem=st_rsem.at[slot],
            device_id={'tp': peer}, device_id_type=MESH)

    peers = [(me + r) % 8 for r in (4, 3, 5, 2, 6, 1, 7)]
    for peer in peers:
        share(peer, me).start()
    blocks = [packed]
    for peer in peers:
        share(peer, peer).wait_recv()
        blocks.append(every[peer])
    ms = [b[:, 0:1] for b in blocks]
    m_all = ms[0]
    for v in ms[1:]:
        m_all = jnp.maximum(m_all, v)
    s_all = jnp.zeros_like(m_all)
    p_all = jnp.zeros_like(m_all)
    for b in blocks:
        s_all = s_all + b[:, 1:2] * jnp.exp(b[:, 0:1] - m_all)
        p_all = p_all + b[:, 2:3]
    log_norm = m_all + jnp.log(s_all)
    stats_ref[...] = jnp.where(lane_id == 0, log_norm, p_all - log_norm)

    def drain(s, carry):
        d2d(s).wait_send()
        return carry
    lax.fori_loop(0, 2 * steps, drain, 0)

    def drain1(i, carry):
        for lane in range(2):
            stage1(lane, i).wait_send()
        return carry
    lax.fori_loop(0, 2 * nl, drain1, 0)

    def drain2(j, carry):
        for lane in range(2):
            stage2(lane, j).wait_send()
        return carry
    lax.fori_loop(0, nl, drain2, 0)
    for peer in peers:
        share(peer, me).wait_send()


def _scores(hidden, gain, table, targets, temperature):
    tokens, hidden_dim = hidden.shape
    vocab, width = table.shape
    rows_per = vocab // 8
    nl = LANE_CHUNKS
    unit = 2 * nl
    need = -(-rows_per // LANES) + 1
    tiles = -(-need // unit) * unit
    chunk = tiles // unit * LANES
    steps = 4 * nl
    f32 = jnp.float32
    dma = pltpu.SemaphoreType.DMA
    block = (tokens, chunk)
    return pl.pallas_call(
        lambda *refs: _kernel((vocab, rows_per, tokens, width, tiles, chunk), *refs),
        out_shape=(jax.ShapeDtypeStruct((tokens, tiles * LANES), f32),
                   jax.ShapeDtypeStruct((tokens, LANES), f32)),
        in_specs=[pl.BlockSpec(memory_space=pltpu.HBM)] * 5,
        out_specs=(pl.BlockSpec(memory_space=pltpu.VMEM), pl.BlockSpec(memory_space=pltpu.VMEM)),
        scratch_shapes=[
            pltpu.VMEM((tokens, hidden_dim), jnp.bfloat16),
            pltpu.VMEM((1, hidden_dim), jnp.bfloat16),
            pltpu.SMEM((tokens,), jnp.int32),
            pltpu.SMEM((1,), f32),
            pltpu.VMEM((tokens, width), jnp.bfloat16),
            pltpu.VMEM((DEPTH * 4, width, chunk), jnp.bfloat16),
            pltpu.VMEM((2 * steps,) + block, f32),
            pltpu.VMEM((2 * steps,) + block, f32),
            pltpu.VMEM((2 * steps,) + block, f32),
            pltpu.VMEM((4 * nl,) + block, f32),
            pltpu.VMEM((2 * nl,) + block, f32),
            pltpu.VMEM((tokens, LANES), f32),
            pltpu.VMEM((8, tokens, LANES), f32),
            dma((4,)), dma((DEPTH * 4,)),
            dma((2 * steps,)), dma((2 * steps,)),
            dma((4 * nl,)), dma((4 * nl,)),
            dma((2 * nl,)), dma((2 * nl,)),
            dma((8,)), dma((8,)),
        ],
        compiler_params=pltpu.CompilerParams(collective_id=0, has_side_effects=True,
                                             vmem_limit_bytes=67043328),
        name='head',
    )(hidden, gain.reshape(1, -1), table.T, targets, temperature.reshape(1))


def solution(mesh):
    def local_scores(hidden, final_gain, table_cols, targets, temperature):
        rows_per = table_cols.shape[0] // 8
        me = lax.axis_index('tp')
        logits, stats = _scores(hidden, final_gain, table_cols, targets, temperature)
        start = me * rows_per - ((me * rows_per) // LANES - me // 7) * LANES
        part = lax.dynamic_slice_in_dim(logits, start, rows_per, axis=1)
        log_norm = stats[:, 0]
        token_probs = jnp.exp(part - stats[:, 0:1]).astype(jnp.bfloat16)
        return log_norm, stats[:, 1], token_probs

    return jax.shard_map(local_scores, mesh=mesh,
                         in_specs=(P('dp', None), P(None), P(None, 'tp'), P('dp'), P()),
                         out_specs=(P('dp'), P('dp'), P('dp', 'tp')),
                         check_vma=False)
```

```python
import jax
import jax.numpy as jnp
from jax import lax
from jax.experimental import pallas as pl
from jax.experimental.pallas import tpu as pltpu
from jax.sharding import PartitionSpec as P

NORM_EPS = 1e-6
LANES = 128
LANE_CHUNKS = 5
DEPTH = 4
NEG = -3.0e38
MESH = pl.DeviceIdType.MESH


def _kernel(shape, hid_hbm, gain_hbm, table_hbm, tgt_hbm, temp, probs_ref, ln_ref, tl_ref,
            hid, gain, gain32, tgt, normed, tbuf, psend, prec, own, r1, r2, logits, shifted, mine, every,
            in_sem, tsem, d2d_ssem, d2d_rsem, s1_ssem, s1_rsem, s2_ssem, s2_rsem, st_ssem, st_rsem):
    rows_per, tokens, width, tiles, chunk = shape
    half_tiles = tiles // 2
    nl = LANE_CHUNKS
    steps = 4 * nl
    me = lax.axis_index('tp')
    core, mx, my = me % 2, (me // 2) % 2, me // 4
    partner = me + 1 - 2 * core
    xn = me + 2 - 4 * mx
    yn = me + 4 - 8 * my
    first = (xn, yn)
    second = (yn, xn)

    def region_tile(d):
        return (d * rows_per) // LANES - d // 7

    def table_copy(i, q):
        p, j = i // nl, i % nl
        lane = q % 2
        a, b = 1 - p // 2, 1 - p % 2
        fx, fy = (a, b) if lane == 0 else (b, a)
        k = 1 - core if q < 2 else core
        d = (my + fy * (1 - 2 * my)) * 4 + (mx + fx * (1 - 2 * mx)) * 2 + k
        tile = region_tile(d) + lane * half_tiles + j * (chunk // LANES)
        col = pl.multiple_of(tile * LANES, LANES)
        slot = (i % DEPTH) * 4 + q
        return pltpu.make_async_copy(table_hbm.at[:, pl.ds(col, chunk)], tbuf.at[slot], tsem.at[slot])

    small = [pltpu.make_async_copy(src, dst, in_sem.at[n]) for n, (src, dst) in enumerate(
        ((hid_hbm, hid), (gain_hbm, gain), (tgt_hbm, tgt)))]
    small[0].start()
    small[1].start()
    for q in range(4):
        table_copy(0, q).start()

    barrier = pltpu.get_barrier_semaphore()
    for r in range(1, 8):
        pl.semaphore_signal(barrier, inc=1, device_id={'tp': (me + r) % 8}, device_id_type=MESH)

    small[0].wait()
    small[1].wait()
    h = hid[...].astype(jnp.float32)
    inv_rms = lax.rsqrt(jnp.mean(h * h, axis=-1, keepdims=True) + NORM_EPS)
    gain32[...] = gain[...].astype(jnp.float32)
    g0 = (me * 3) // 2
    hc = hid[:, pl.ds(pl.multiple_of(g0 * LANES, LANES), 2 * LANES)].astype(jnp.float32)
    u0 = hc[:, :LANES] * inv_rms * gain32[pl.ds(g0, 1), :]
    u1 = hc[:, LANES:] * inv_rms * gain32[pl.ds(g0 + 1, 1), :]
    u = jnp.concatenate([u0, u1], axis=1)
    u = jnp.where(core == 0, u[:, :width], u[:, 2 * LANES - width:])
    normed[...] = u.astype(jnp.bfloat16)

    for i in range(1, DEPTH):
        for q in range(4):
            table_copy(i, q).start()
    small[2].start()

    pl.semaphore_wait(barrier, 7)

    def d2d(s):
        return pltpu.make_async_remote_copy(
            src_ref=psend.at[s], dst_ref=prec.at[s], send_sem=d2d_ssem.at[s], recv_sem=d2d_rsem.at[s],
            device_id={'tp': partner}, device_id_type=MESH)

    def stage1(lane, i):
        s = i * 2 + lane
        return pltpu.make_async_remote_copy(
            src_ref=own.at[s], dst_ref=r1.at[s], send_sem=s1_ssem.at[s], recv_sem=s1_rsem.at[s],
            device_id={'tp': first[lane]}, device_id_type=MESH)

    def stage2(lane, j):
        s = j * 2 + lane
        return pltpu.make_async_remote_copy(
            src_ref=own.at[4 * nl + s], dst_ref=r2.at[s], send_sem=s2_ssem.at[s], recv_sem=s2_rsem.at[s],
            device_id={'tp': second[lane]}, device_id_type=MESH)

    def compute(i, qs, prefetch):
        for q in qs:
            s = i * 2 + q % 2
            slot = (i % DEPTH) * 4 + q
            table_copy(i, q).wait()
            out = psend if q < 2 else own
            out[s] = jnp.dot(normed[...], tbuf[slot], preferred_element_type=jnp.float32)
            if q < 2:
                d2d(s).start()
            if prefetch is None:
                @pl.when(i + DEPTH < steps)
                def _():
                    table_copy(i + DEPTH, q).start()
            elif prefetch:
                table_copy(i + DEPTH, q).start()

    theirs, ours = (0, 1), (2, 3)

    def gather_pair(i, send):
        for lane in range(2):
            s = i * 2 + lane
            d2d(s).wait_recv()
            own[s] = own[s] + prec[s]
            if send:
                stage1(lane, i).start()

    compute(0, theirs, True)
    compute(0, ours, True)
    compute(1, theirs, True)

    def loop_send(i, carry):
        gather_pair(i, True)
        compute(i + 1, ours, True)
        compute(i + 2, theirs, True)
        return carry

    def loop_keep(i, carry):
        gather_pair(i, False)
        compute(i + 1, ours, None)
        compute(i + 2, theirs, None)
        return carry

    lax.fori_loop(0, 2 * nl, loop_send, 0)
    lax.fori_loop(2 * nl, steps - 2, loop_keep, 0)
    gather_pair(steps - 2, False)
    compute(steps - 1, ours, False)
    gather_pair(steps - 1, False)

    def forward(j, carry):
        for lane in range(2):
            stage1(lane, j).wait_recv()
            s = (2 * nl + j) * 2 + lane
            own[s] = own[s] + r1[j * 2 + lane]
            stage2(lane, j).start()
        return carry

    lax.fori_loop(0, nl, forward, 0)

    small[2].wait()
    temperature = temp[0]
    row = lax.broadcasted_iota(jnp.int32, (tokens, LANES), 0)
    lane_id = lax.broadcasted_iota(jnp.int32, (tokens, LANES), 1)
    target = jnp.zeros((tokens, LANES), jnp.int32)
    for t in range(tokens):
        target = jnp.where(row == t, tgt[t], target)
    lo = me * rows_per
    base = region_tile(me) * LANES

    def finish(j, carry):
        m, total, picked = carry
        for lane in range(2):
            stage1(lane, nl + j).wait_recv()
            stage2(lane, j).wait_recv()
            z = own[(3 * nl + j) * 2 + lane] + r1[(nl + j) * 2 + lane] + r2[j * 2 + lane]
            t = z / temperature
            off = pl.multiple_of((lane * half_tiles + j * (chunk // LANES)) * LANES, LANES)
            logits[:, pl.ds(off, chunk)] = t
            parts = []
            top = m
            for k in range(chunk // LANES):
                piece = t[:, k * LANES:(k + 1) * LANES]
                col = lane_id + (base + off + k * LANES)
                inside = (col >= lo) & (col < lo + rows_per)
                piece_in = jnp.where(inside, piece, NEG)
                picked = picked + jnp.where(inside & (col == target), piece, 0.0)
                parts.append(piece_in)
                top = jnp.maximum(top, piece_in)
            total = total * jnp.exp(m - top)
            for piece_in in parts:
                total = total + jnp.exp(piece_in - top)
            m = top
        return m, total, picked

    m, total, picked = lax.fori_loop(
        0, nl, finish,
        (jnp.full((tokens, LANES), NEG, jnp.float32), jnp.zeros((tokens, LANES), jnp.float32),
         jnp.zeros((tokens, LANES), jnp.float32)))
    m_row = jnp.max(m, axis=-1, keepdims=True)
    s_row = jnp.sum(total * jnp.exp(m - m_row), axis=-1, keepdims=True)
    p_row = jnp.sum(picked, axis=-1, keepdims=True)
    hs = tokens // 2
    lane8 = lax.broadcasted_iota(jnp.int32, (hs, LANES), 1)
    packed = jnp.broadcast_to(p_row[hs:], (hs, LANES))
    for n, v in enumerate((m_row[:hs], m_row[hs:], s_row[:hs], s_row[hs:], p_row[:hs])):
        packed = jnp.where(lane8 == n, v, packed)
    mine[...] = packed

    def share(peer, slot):
        return pltpu.make_async_remote_copy(
            src_ref=mine, dst_ref=every.at[slot], send_sem=st_ssem.at[peer], recv_sem=st_rsem.at[slot],
            device_id={'tp': peer}, device_id_type=MESH)

    far = me + 6 - 4 * mx - 8 * my + 0 * core
    peers = [far, far + 1 - 2 * core, yn, yn + 1 - 2 * core, xn, xn + 1 - 2 * core, partner]
    for peer in peers:
        share(peer, me).start()

    shift = lo - base
    skip, turn = shift // LANES, shift % LANES
    rot = (LANES - turn) % LANES
    out_tiles = -(-rows_per // LANES)
    keep = lane_id < LANES - turn

    def turned(k):
        at = pl.multiple_of((skip + k) * LANES, LANES)
        return pltpu.roll(logits[:, pl.ds(at, LANES)], rot, axis=1)

    cur = turned(0)
    for k in range(out_tiles):
        if k + 1 < out_tiles:
            nxt = turned(k + 1)
        else:
            nxt = pltpu.roll(logits[:, (tiles - 1) * LANES:tiles * LANES], rot, axis=1)
        shifted[:, k * LANES:(k + 1) * LANES] = jnp.where(keep, cur, nxt)
        cur = nxt

    def drain(s, carry):
        d2d(s).wait_send()
        return carry
    lax.fori_loop(0, 2 * steps, drain, 0)

    def drain1(i, carry):
        for lane in range(2):
            stage1(lane, i).wait_send()
        return carry
    lax.fori_loop(0, 2 * nl, drain1, 0)

    def drain2(j, carry):
        for lane in range(2):
            stage2(lane, j).wait_send()
        return carry
    lax.fori_loop(0, nl, drain2, 0)

    blocks = [packed]
    for peer in reversed(peers):
        share(peer, peer).wait_recv()
        blocks.append(every[peer])

    def rows16(n):
        return [jnp.concatenate([b[:, n:n + 1], b[:, n + 1:n + 2]], axis=0) for b in blocks]

    ms, ss, ps = rows16(0), rows16(2), rows16(4)
    m_all = ms[0]
    for v in ms[1:]:
        m_all = jnp.maximum(m_all, v)
    s_all = jnp.zeros_like(m_all)
    p_all = jnp.zeros_like(m_all)
    for mv, sv, pv in zip(ms, ss, ps):
        s_all = s_all + sv * jnp.exp(mv - m_all)
        p_all = p_all + pv
    log_norm = m_all + jnp.log(s_all)

    step = 19 * LANES
    for at in range(0, rows_per, step):
        end = min(at + step, rows_per)
        probs_ref[:, at:end] = jnp.exp(shifted[:, at:end] - log_norm).astype(jnp.bfloat16)

    def as_row(v):
        spread = jnp.where(lane_id == row, jnp.broadcast_to(v, (tokens, LANES)), 0.0)
        return jnp.sum(spread, axis=0, keepdims=True)[:, :tokens]
    ln_ref[...] = as_row(log_norm)
    tl_ref[...] = as_row(p_all - log_norm)
    for peer in peers:
        share(peer, me).wait_send()


def _scores(hidden, gain, table, targets, temperature):
    tokens, hidden_dim = hidden.shape
    vocab, width = table.shape
    rows_per = vocab // 8
    nl = LANE_CHUNKS
    unit = 2 * nl
    need = -(-rows_per // LANES) + 1
    tiles = -(-need // unit) * unit
    chunk = tiles // unit * LANES
    steps = 4 * nl
    out_tiles = -(-rows_per // LANES)
    f32 = jnp.float32
    dma = pltpu.SemaphoreType.DMA
    block = (tokens, chunk)
    grows = hidden_dim // LANES
    hbm = lambda v: pltpu.with_memory_space_constraint(v, pltpu.HBM)
    return pl.pallas_call(
        lambda *refs: _kernel((rows_per, tokens, width, tiles, chunk), *refs),
        out_shape=(pltpu.VMEM((tokens, rows_per), jnp.bfloat16),
                   pltpu.VMEM((1, tokens), f32), pltpu.VMEM((1, tokens), f32)),
        in_specs=[pl.BlockSpec(memory_space=pltpu.HBM)] * 4 + [pl.BlockSpec(memory_space=pltpu.SMEM)],
        out_specs=(pl.BlockSpec(memory_space=pltpu.VMEM),) * 3,
        scratch_shapes=[
            pltpu.VMEM((tokens, hidden_dim), jnp.bfloat16),
            pltpu.VMEM((grows, LANES), jnp.bfloat16),
            pltpu.VMEM((grows, LANES), f32),
            pltpu.SMEM((tokens,), jnp.int32),
            pltpu.VMEM((tokens, width), jnp.bfloat16),
            pltpu.VMEM((DEPTH * 4, width, chunk), jnp.bfloat16),
            pltpu.VMEM((2 * steps,) + block, f32),
            pltpu.VMEM((2 * steps,) + block, f32),
            pltpu.VMEM((2 * steps,) + block, f32),
            pltpu.VMEM((4 * nl,) + block, f32),
            pltpu.VMEM((2 * nl,) + block, f32),
            pltpu.VMEM((tokens, tiles * LANES), f32),
            pltpu.VMEM((tokens, out_tiles * LANES), f32),
            pltpu.VMEM((tokens // 2, LANES), f32),
            pltpu.VMEM((8, tokens // 2, LANES), f32),
            dma((3,)), dma((DEPTH * 4,)),
            dma((2 * steps,)), dma((2 * steps,)),
            dma((4 * nl,)), dma((4 * nl,)),
            dma((2 * nl,)), dma((2 * nl,)),
            dma((8,)), dma((8,)),
        ],
        compiler_params=pltpu.CompilerParams(collective_id=0, has_side_effects=True,
                                             vmem_limit_bytes=48 * 1024 * 1024),
        name='head',
    )(hbm(hidden), hbm(gain.reshape(grows, LANES)), hbm(table.T), hbm(targets), temperature.reshape(1))


def solution(mesh):
    def local_scores(hidden, final_gain, table_cols, targets, temperature):
        probs, ln, tl = _scores(hidden, final_gain, table_cols, targets, temperature)
        return ln.reshape(-1), tl.reshape(-1), probs

    return jax.shard_map(local_scores, mesh=mesh,
                         in_specs=(P('dp', None), P(None), P(None, 'tp'), P('dp'), P()),
                         out_specs=(P('dp'), P('dp'), P('dp', 'tp')),
                         check_vma=False)
```

```python
import jax
import jax.numpy as jnp
from jax import lax
from jax.experimental import pallas as pl
from jax.experimental.pallas import tpu as pltpu
from jax.sharding import PartitionSpec as P

NORM_EPS = 1e-6
LANES = 128
LANE_CHUNKS = 5
DEPTH = 4
HEAD = 5 * LANES
NEG = -3.0e38
MESH = pl.DeviceIdType.MESH


def _kernel(shape, hid_hbm, gain_hbm, table_hbm, tgt_hbm, temp, shifted, blocks_ref,
            hid, gain, gain32, tgt, normed, tbuf, psend, prec, own, r1, r2, logits, mine, every,
            in_sem, tsem, head_sem, d2d_rsem, s1_rsem, s2_rsem, st_rsem, out_sem):
    rows_per, tokens, width, tiles, chunk = shape
    half_tiles = tiles // 2
    nl = LANE_CHUNKS
    steps = 4 * nl
    me = lax.axis_index('tp')
    core, mx, my = me % 2, (me // 2) % 2, me // 4
    partner = me + 1 - 2 * core
    xn = me + 2 - 4 * mx
    yn = me + 4 - 8 * my
    first = (xn, yn)
    second = (yn, xn)

    def region_tile(d):
        return (d * rows_per) // LANES - d // 7

    def table_copy(i, q, cut=None):
        p, j = i // nl, i % nl
        lane = q % 2
        a, b = 1 - p // 2, 1 - p % 2
        fx, fy = (a, b) if lane == 0 else (b, a)
        k = 1 - core if q < 2 else core
        d = (my + fy * (1 - 2 * my)) * 4 + (mx + fx * (1 - 2 * mx)) * 2 + k
        tile = region_tile(d) + lane * half_tiles + j * (chunk // LANES)
        col = pl.multiple_of(tile * LANES, LANES)
        slot = (i % DEPTH) * 4 + q
        if cut is None:
            return pltpu.make_async_copy(table_hbm.at[:, pl.ds(col, chunk)], tbuf.at[slot],
                                         tsem.at[slot // 2])
        lo, hi, sem = cut
        return pltpu.make_async_copy(table_hbm.at[:, pl.ds(col + lo, hi - lo)],
                                     tbuf.at[slot, :, pl.ds(lo, hi - lo)], sem)

    small = [pltpu.make_async_copy(src, dst, in_sem.at[n]) for n, (src, dst) in enumerate(
        ((hid_hbm, hid), (gain_hbm, gain), (tgt_hbm, tgt)))]
    small[1].start()
    small[0].start()
    for q in range(2):
        table_copy(0, q, (0, HEAD, head_sem.at[q])).start()
    for q in range(2):
        table_copy(0, q, (HEAD, chunk, tsem.at[0])).start()
    for q in range(2, 4):
        table_copy(0, q).start()

    barrier = pltpu.get_barrier_semaphore()
    for peer in (partner, xn, yn):
        pl.semaphore_signal(barrier, inc=1, device_id={'tp': peer}, device_id_type=MESH)

    small[0].wait()
    h = hid[...].astype(jnp.float32)
    inv_rms = lax.rsqrt(jnp.mean(h * h, axis=-1, keepdims=True) + NORM_EPS)
    small[1].wait()
    gain32[...] = gain[...].astype(jnp.float32)
    g0 = (me * 3) // 2
    hc = hid[:, pl.ds(pl.multiple_of(g0 * LANES, LANES), 2 * LANES)].astype(jnp.float32)
    u0 = hc[:, :LANES] * inv_rms * gain32[pl.ds(g0, 1), :]
    u1 = hc[:, LANES:] * inv_rms * gain32[pl.ds(g0 + 1, 1), :]
    u = jnp.concatenate([u0, u1], axis=1)
    u = jnp.where(core == 0, u[:, :width], u[:, 2 * LANES - width:])
    normed[...] = u.astype(jnp.bfloat16)

    for i in range(1, DEPTH):
        for q in range(4):
            table_copy(i, q).start()
    small[2].start()

    pl.semaphore_wait(barrier, 3)

    def remote(src, dst, kind, recv, device):
        return pltpu.make_async_remote_copy(src_ref=src, dst_ref=dst, send_sem=out_sem.at[kind], recv_sem=recv,
                                            device_id={'tp': device}, device_id_type=MESH)

    def d2d(i, lane):
        return remote(psend.at[i, lane], prec.at[i, lane], 0, d2d_rsem.at[i], partner)

    def d2d_part(lane, lo, hi, sem):
        at = pl.ds(lo, hi - lo)
        return remote(psend.at[0, lane, :, at], prec.at[0, lane, :, at], 0, sem, partner)

    def stage1(lane, i):
        return remote(own.at[i, lane], r1.at[i, lane], 1, s1_rsem.at[i], first[lane])

    def stage1_part(lane, lo, hi):
        at = pl.ds(lo, hi - lo)
        return remote(own.at[0, lane, :, at], r1.at[0, lane, :, at], 1, s1_rsem.at[0], first[lane])

    def stage2(lane, j):
        return remote(own.at[2 * nl + j, lane], r2.at[j, lane], 2, s2_rsem.at[j], second[lane])

    def d2d_pair(i):
        return remote(psend.at[i], prec.at[i], 0, d2d_rsem.at[i], partner)

    def stage1_pair(i):
        return remote(own.at[i], r1.at[i], 1, s1_rsem.at[i], xn)

    def stage2_pair(j):
        return remote(own.at[2 * nl + j], r2.at[j], 2, s2_rsem.at[j], yn)

    def multiply(i, q, cols=slice(None)):
        out = psend if q < 2 else own
        slot = (i % DEPTH) * 4 + q
        out[i, q % 2, :, cols] = jnp.dot(normed[...], tbuf[slot, :, cols], preferred_element_type=jnp.float32)

    def pair_wait(i, half):
        slot = (i % DEPTH) * 4 + half * 2
        both = tbuf.at[pl.ds(slot, 2)]
        pltpu.make_async_copy(both, both, tsem.at[slot // 2]).wait()

    def compute(i, qs, prefetch):
        pair_wait(i, qs[0] // 2)
        for q in qs:
            multiply(i, q)
            if q < 2:
                d2d(i, q).start()
            if prefetch is None:
                @pl.when(i + DEPTH < steps)
                def _():
                    table_copy(i + DEPTH, q).start()
            elif prefetch:
                table_copy(i + DEPTH, q).start()

    theirs, ours = (0, 1), (2, 3)

    def gather_pair(i, send):
        d2d_pair(i).wait_recv()
        for lane in range(2):
            own[i, lane] = own[i, lane] + prec[i, lane]
            if send:
                stage1(lane, i).start()

    for q in range(2):
        table_copy(0, q, (0, HEAD, head_sem.at[q])).wait()
        multiply(0, q, slice(0, HEAD))
        d2d_part(q, 0, HEAD, head_sem.at[2 + q]).start()
    rest = tbuf.at[pl.ds(0, 2), :, pl.ds(HEAD, chunk - HEAD)]
    pltpu.make_async_copy(rest, rest, tsem.at[0]).wait()
    for q in range(2):
        multiply(0, q, slice(HEAD, chunk))
        d2d_part(q, HEAD, chunk, d2d_rsem.at[0]).start()
        table_copy(DEPTH, q).start()
    compute(0, ours, True)
    for lane in range(2):
        d2d_part(lane, 0, HEAD, head_sem.at[2 + lane]).wait_recv()
        own[0, lane, :, :HEAD] = own[0, lane, :, :HEAD] + prec[0, lane, :, :HEAD]
        stage1_part(lane, 0, HEAD).start()
    compute(1, theirs, True)
    tail = pl.ds(HEAD, chunk - HEAD)
    remote(psend.at[0, :, :, tail], prec.at[0, :, :, tail], 0, d2d_rsem.at[0], partner).wait_recv()
    for lane in range(2):
        own[0, lane, :, HEAD:] = own[0, lane, :, HEAD:] + prec[0, lane, :, HEAD:]
        stage1_part(lane, HEAD, chunk).start()
    compute(1, ours, True)
    compute(2, theirs, True)

    def loop_send(i, carry):
        gather_pair(i, True)
        compute(i + 1, ours, True)
        compute(i + 2, theirs, True)
        return carry

    def loop_keep(i, carry):
        gather_pair(i, False)
        compute(i + 1, ours, None)
        compute(i + 2, theirs, None)
        return carry

    lax.fori_loop(1, 2 * nl, loop_send, 0)
    lax.fori_loop(2 * nl, steps - 2, loop_keep, 0)
    gather_pair(steps - 2, False)
    compute(steps - 1, ours, False)
    gather_pair(steps - 1, False)

    def forward(j, carry):
        stage1_pair(j).wait_recv()
        for lane in range(2):
            own[2 * nl + j, lane] = own[2 * nl + j, lane] + r1[j, lane]
            stage2(lane, j).start()
        return carry

    lax.fori_loop(0, nl, forward, 0)

    small[2].wait()
    temperature = temp[0]
    row = lax.broadcasted_iota(jnp.int32, (tokens, LANES), 0)
    lane_id = lax.broadcasted_iota(jnp.int32, (tokens, LANES), 1)
    target = jnp.zeros((tokens, LANES), jnp.int32)
    for t in range(tokens):
        target = jnp.where(row == t, tgt[t], target)
    lo = me * rows_per
    base = region_tile(me) * LANES

    def finish(j, carry):
        m, total, picked = carry
        stage1_pair(nl + j).wait_recv()
        stage2_pair(j).wait_recv()
        for lane in range(2):
            z = own[3 * nl + j, lane] + r1[nl + j, lane] + r2[j, lane]
            t = z / temperature
            off = pl.multiple_of((lane * half_tiles + j * (chunk // LANES)) * LANES, LANES)
            logits[:, pl.ds(off, chunk)] = t
            parts = []
            top = m
            for k in range(chunk // LANES):
                piece = t[:, k * LANES:(k + 1) * LANES]
                col = lane_id + (base + off + k * LANES)
                inside = (col >= lo) & (col < lo + rows_per)
                piece_in = jnp.where(inside, piece, NEG)
                picked = picked + jnp.where(inside & (col == target), piece, 0.0)
                parts.append(piece_in)
                top = jnp.maximum(top, piece_in)
            total = total * jnp.exp(m - top)
            for piece_in in parts:
                total = total + jnp.exp(piece_in - top)
            m = top
        return m, total, picked

    m, total, picked = lax.fori_loop(
        0, nl, finish,
        (jnp.full((tokens, LANES), NEG, jnp.float32), jnp.zeros((tokens, LANES), jnp.float32),
         jnp.zeros((tokens, LANES), jnp.float32)))
    m_row = jnp.max(m, axis=-1, keepdims=True)
    s_row = jnp.sum(total * jnp.exp(m - m_row), axis=-1, keepdims=True)
    p_row = jnp.sum(picked, axis=-1, keepdims=True)
    hs = tokens // 2
    lane8 = lax.broadcasted_iota(jnp.int32, (hs, LANES), 1)
    packed = jnp.broadcast_to(p_row[hs:], (hs, LANES))
    for n, v in enumerate((m_row[:hs], m_row[hs:], s_row[:hs], s_row[hs:], p_row[:hs])):
        packed = jnp.where(lane8 == n, v, packed)
    mine[...] = packed

    def share(peer):
        return remote(mine, every.at[me], 3, st_rsem.at[0], peer)

    far = me + 6 - 4 * mx - 8 * my
    peers = [far, far + 1 - 2 * core, yn, yn + 1 - 2 * core, xn, xn + 1 - 2 * core, partner]
    every[me] = packed
    for peer in peers:
        share(peer).start()

    shift = lo - base
    skip, turn = shift // LANES, shift % LANES
    rot = (LANES - turn) % LANES
    out_tiles = -(-rows_per // LANES)
    keep = lane_id < LANES - turn

    def turned(k):
        at = pl.multiple_of((skip + k) * LANES, LANES)
        return pltpu.roll(logits[:, pl.ds(at, LANES)], rot, axis=1)

    cur = turned(0)
    for k in range(out_tiles):
        if k + 1 < out_tiles:
            nxt = turned(k + 1)
        else:
            nxt = pltpu.roll(logits[:, (tiles - 1) * LANES:tiles * LANES], rot, axis=1)
        shifted[:, k * LANES:(k + 1) * LANES] = jnp.where(keep, cur, nxt)
        cur = nxt

    remote(psend, prec, 0, d2d_rsem.at[0], partner).wait_send()
    sent1 = own.at[pl.ds(0, 2 * nl)]
    remote(sent1, r1, 1, s1_rsem.at[0], xn).wait_send()
    sent2 = own.at[pl.ds(2 * nl, nl)]
    remote(sent2, r2, 2, s2_rsem.at[0], yn).wait_send()

    seven = every.at[pl.ds(0, 7)]
    remote(seven, seven, 3, st_rsem.at[0], partner).wait_recv()
    blocks_ref[...] = every[...]
    remote(seven, seven, 3, st_rsem.at[0], partner).wait_send()


def _finish_kernel(tokens, rows_per, shifted, blocks_ref, probs_hbm, ln_hbm, tl_hbm, probs, ln, tl, sem):
    row = lax.broadcasted_iota(jnp.int32, (tokens, LANES), 0)
    lane_id = lax.broadcasted_iota(jnp.int32, (tokens, LANES), 1)
    blocks = [blocks_ref[d] for d in range(8)]

    def rows16(n):
        return [jnp.concatenate([b[:, n:n + 1], b[:, n + 1:n + 2]], axis=0) for b in blocks]

    ms, ss, ps = rows16(0), rows16(2), rows16(4)
    m_all = ms[0]
    for v in ms[1:]:
        m_all = jnp.maximum(m_all, v)
    s_all = jnp.zeros_like(m_all)
    p_all = jnp.zeros_like(m_all)
    for mv, sv, pv in zip(ms, ss, ps):
        s_all = s_all + sv * jnp.exp(mv - m_all)
        p_all = p_all + pv
    log_norm = m_all + jnp.log(s_all)

    def as_row(v):
        spread = jnp.where(lane_id == row, jnp.broadcast_to(v, (tokens, LANES)), 0.0)
        return jnp.sum(spread, axis=0, keepdims=True)[:, :tokens]
    ln[...] = as_row(log_norm)
    tl[...] = as_row(p_all - log_norm)
    copies = [pltpu.make_async_copy(ln, ln_hbm, sem.at[0]), pltpu.make_async_copy(tl, tl_hbm, sem.at[1])]
    for c in copies:
        c.start()

    step = 19 * LANES
    for at in range(0, rows_per, step):
        end = min(at + step, rows_per)
        probs[:, at:end] = jnp.exp(shifted[:, at:end] - log_norm).astype(jnp.bfloat16)
    copies.append(pltpu.make_async_copy(probs, probs_hbm, sem.at[2]))
    copies[-1].start()
    for c in copies:
        c.wait()


def _scores(hidden, gain, table, targets, temperature):
    tokens, hidden_dim = hidden.shape
    vocab, width = table.shape
    rows_per = vocab // 8
    nl = LANE_CHUNKS
    unit = 2 * nl
    need = -(-rows_per // LANES) + 1
    tiles = -(-need // unit) * unit
    chunk = tiles // unit * LANES
    steps = 4 * nl
    out_tiles = -(-rows_per // LANES)
    f32 = jnp.float32
    dma = pltpu.SemaphoreType.DMA
    block = (tokens, chunk)
    grows = hidden_dim // LANES
    hbm = lambda v: pltpu.with_memory_space_constraint(v, pltpu.HBM)
    shifted, blocks = pl.pallas_call(
        lambda *refs: _kernel((rows_per, tokens, width, tiles, chunk), *refs),
        out_shape=(pltpu.VMEM((tokens, out_tiles * LANES), f32), pltpu.VMEM((8, tokens // 2, LANES), f32)),
        in_specs=[pl.BlockSpec(memory_space=pltpu.HBM)] * 4 + [pl.BlockSpec(memory_space=pltpu.SMEM)],
        out_specs=(pl.BlockSpec(memory_space=pltpu.VMEM),) * 2,
        scratch_shapes=[
            pltpu.VMEM((tokens, hidden_dim), jnp.bfloat16),
            pltpu.VMEM((grows, LANES), jnp.bfloat16),
            pltpu.VMEM((grows, LANES), f32),
            pltpu.SMEM((tokens,), jnp.int32),
            pltpu.VMEM((tokens, width), jnp.bfloat16),
            pltpu.VMEM((DEPTH * 4, width, chunk), jnp.bfloat16),
            pltpu.VMEM((steps, 2) + block, f32),
            pltpu.VMEM((steps, 2) + block, f32),
            pltpu.VMEM((steps, 2) + block, f32),
            pltpu.VMEM((2 * nl, 2) + block, f32),
            pltpu.VMEM((nl, 2) + block, f32),
            pltpu.VMEM((tokens, tiles * LANES), f32),
            pltpu.VMEM((tokens // 2, LANES), f32),
            pltpu.VMEM((8, tokens // 2, LANES), f32),
            dma((3,)), dma((DEPTH * 2,)), dma((4,)),
            dma((steps,)), dma((2 * nl,)), dma((nl,)), dma((1,)), dma((4,)),
        ],
        compiler_params=pltpu.CompilerParams(collective_id=0, has_side_effects=True,
                                             vmem_limit_bytes=48 * 1024 * 1024),
        name='head',
    )(hbm(hidden), hbm(gain.reshape(grows, LANES)), hbm(table.T), hbm(targets), temperature.reshape(1))
    return pl.pallas_call(
        lambda *refs: _finish_kernel(tokens, rows_per, *refs),
        out_shape=(jax.ShapeDtypeStruct((tokens, rows_per), jnp.bfloat16),
                   jax.ShapeDtypeStruct((1, tokens), f32), jax.ShapeDtypeStruct((1, tokens), f32)),
        in_specs=[pl.BlockSpec(memory_space=pltpu.VMEM)] * 2,
        out_specs=(pl.BlockSpec(memory_space=pltpu.HBM),) * 3,
        scratch_shapes=[pltpu.VMEM((tokens, rows_per), jnp.bfloat16), pltpu.VMEM((1, tokens), f32),
                        pltpu.VMEM((1, tokens), f32), dma((3,))],
        compiler_params=pltpu.CompilerParams(vmem_limit_bytes=16 * 1024 * 1024),
        name='finish',
    )(shifted, blocks)


def solution(mesh):
    def local_scores(hidden, final_gain, table_cols, targets, temperature):
        probs, ln, tl = _scores(hidden, final_gain, table_cols, targets, temperature)
        return ln.reshape(-1), tl.reshape(-1), probs

    return jax.shard_map(local_scores, mesh=mesh,
                         in_specs=(P('dp', None), P(None), P(None, 'tp'), P('dp'), P()),
                         out_specs=(P('dp'), P('dp'), P('dp', 'tp')),
                         check_vma=False)
```

```python
import jax
import jax.numpy as jnp
from jax import lax
from jax.experimental import pallas as pl
from jax.experimental.pallas import tpu as pltpu
from jax.sharding import PartitionSpec as P

NORM_EPS = 1e-6
LANES = 128
LANE_CHUNKS = 5
DEPTH = 4
HEAD = 5 * LANES
NEG = -3.0e38
MESH = pl.DeviceIdType.MESH


def _kernel(shape, hid_hbm, gain_hbm, table_hbm, tgt_hbm, temp, shifted, blocks_ref,
            hid, gain, gain32, tgt, normed, tbuf, psend, prec, own, r1, r2, logits, mine, every,
            in_sem, tsem, head_sem, d2d_rsem, s1_rsem, s2_rsem, st_rsem, out_sem):
    rows_per, tokens, width, tiles, chunk = shape
    half_tiles = tiles // 2
    nl = LANE_CHUNKS
    steps = 4 * nl
    me = lax.axis_index('tp')
    core, mx, my = me % 2, (me // 2) % 2, me // 4
    partner = me + 1 - 2 * core
    xn = me + 2 - 4 * mx
    yn = me + 4 - 8 * my
    first = (xn, yn)
    second = (yn, xn)

    def region_tile(d):
        return (d * rows_per) // LANES - d // 7

    def table_copy(i, q, cut=None):
        p, j = i // nl, i % nl
        lane = q % 2
        a, b = 1 - p // 2, 1 - p % 2
        fx, fy = (a, b) if lane == 0 else (b, a)
        k = 1 - core if q < 2 else core
        d = (my + fy * (1 - 2 * my)) * 4 + (mx + fx * (1 - 2 * mx)) * 2 + k
        tile = region_tile(d) + lane * half_tiles + j * (chunk // LANES)
        col = pl.multiple_of(tile * LANES, LANES)
        slot = (i % DEPTH) * 4 + q
        if cut is None:
            return pltpu.make_async_copy(table_hbm.at[:, pl.ds(col, chunk)], tbuf.at[slot],
                                         tsem.at[slot // 2])
        lo, hi, sem = cut
        return pltpu.make_async_copy(table_hbm.at[:, pl.ds(col + lo, hi - lo)],
                                     tbuf.at[slot, :, pl.ds(lo, hi - lo)], sem)

    small = [pltpu.make_async_copy(src, dst, in_sem.at[n]) for n, (src, dst) in enumerate(
        ((hid_hbm, hid), (gain_hbm, gain), (tgt_hbm, tgt)))]
    small[0].start()
    small[1].start()
    for q in range(4):
        table_copy(0, q, (0, HEAD, head_sem.at[min(q, 2)])).start()

    barrier = pltpu.get_barrier_semaphore()
    for peer in (partner, xn, yn):
        pl.semaphore_signal(barrier, inc=1, device_id={'tp': peer}, device_id_type=MESH)

    small[0].wait()
    for q in range(4):
        table_copy(0, q, (HEAD, chunk, tsem.at[q // 2])).start()
    h = hid[...].astype(jnp.float32)
    inv_rms = lax.rsqrt(jnp.mean(h * h, axis=-1, keepdims=True) + NORM_EPS)
    small[1].wait()
    gain32[...] = gain[...].astype(jnp.float32)
    g0 = (me * 3) // 2
    hc = hid[:, pl.ds(pl.multiple_of(g0 * LANES, LANES), 2 * LANES)].astype(jnp.float32)
    u0 = hc[:, :LANES] * inv_rms * gain32[pl.ds(g0, 1), :]
    u1 = hc[:, LANES:] * inv_rms * gain32[pl.ds(g0 + 1, 1), :]
    u = jnp.concatenate([u0, u1], axis=1)
    u = jnp.where(core == 0, u[:, :width], u[:, 2 * LANES - width:])
    normed[...] = u.astype(jnp.bfloat16)

    pl.semaphore_wait(barrier, 3)

    def remote(src, dst, kind, recv, device):
        return pltpu.make_async_remote_copy(src_ref=src, dst_ref=dst, send_sem=out_sem.at[kind], recv_sem=recv,
                                            device_id={'tp': device}, device_id_type=MESH)

    def d2d(i, lane):
        return remote(psend.at[i, lane], prec.at[i, lane], 0, d2d_rsem.at[i - (i // (2 * nl)) * (i - 2 * nl)], partner)

    def d2d_part(lane, lo, hi, sem):
        at = pl.ds(lo, hi - lo)
        return remote(psend.at[0, lane, :, at], prec.at[0, lane, :, at], 0, sem, partner)

    def stage1(lane, i):
        return remote(own.at[i, lane], r1.at[i, lane], 1, s1_rsem.at[i // nl], first[lane])

    def stage1_part(lane, lo, hi):
        at = pl.ds(lo, hi - lo)
        return remote(own.at[0, lane, :, at], r1.at[0, lane, :, at], 1, s1_rsem.at[0], first[lane])

    def stage2(lane, j):
        return remote(own.at[2 * nl + j, lane], r2.at[j, lane], 2, s2_rsem.at[j], second[lane])

    def d2d_pair(i):
        return remote(psend.at[i], prec.at[i], 0, d2d_rsem.at[i], partner)

    def stage2_pair(j):
        return remote(own.at[2 * nl + j], r2.at[j], 2, s2_rsem.at[j], yn)

    def multiply(i, q, cols=slice(None)):
        out = psend if q < 2 else own
        slot = (i % DEPTH) * 4 + q
        out[i, q % 2, :, cols] = jnp.dot(normed[...], tbuf[slot, :, cols], preferred_element_type=jnp.float32)

    def pair_wait(i, half):
        slot = (i % DEPTH) * 4 + half * 2
        both = tbuf.at[pl.ds(slot, 2)]
        pltpu.make_async_copy(both, both, tsem.at[slot // 2]).wait()

    def compute(i, qs, prefetch):
        pair_wait(i, qs[0] // 2)
        for q in qs:
            multiply(i, q)
            if q < 2:
                d2d(i, q).start()
            if prefetch is None:
                @pl.when(i + DEPTH < steps)
                def _():
                    table_copy(i + DEPTH, q).start()
            elif prefetch:
                table_copy(i + DEPTH, q).start()

    theirs, ours = (0, 1), (2, 3)

    def piece(half, lo, hi):
        return tbuf.at[pl.ds(2 * half, 2), :, pl.ds(lo, hi - lo)]

    for q in range(2):
        table_copy(0, q, (0, HEAD, head_sem.at[q])).wait()
        multiply(0, q, slice(0, HEAD))
        d2d_part(q, 0, HEAD, head_sem.at[3 + q]).start()
    pltpu.make_async_copy(piece(1, 0, HEAD), piece(1, 0, HEAD), head_sem.at[2]).wait()
    for q in range(2, 4):
        multiply(0, q, slice(0, HEAD))
    for i in range(1, DEPTH):
        for q in range(4):
            table_copy(i, q).start()
    small[2].start()
    pltpu.make_async_copy(piece(0, HEAD, chunk), piece(0, HEAD, chunk), tsem.at[0]).wait()
    for q in range(2):
        multiply(0, q, slice(HEAD, chunk))
        d2d_part(q, HEAD, chunk, d2d_rsem.at[0]).start()
        table_copy(DEPTH, q).start()
    for lane in range(2):
        d2d_part(lane, 0, HEAD, head_sem.at[3 + lane]).wait_recv()
        own[0, lane, :, :HEAD] = own[0, lane, :, :HEAD] + prec[0, lane, :, :HEAD]
        stage1_part(lane, 0, HEAD).start()
    pltpu.make_async_copy(piece(1, HEAD, chunk), piece(1, HEAD, chunk), tsem.at[1]).wait()
    for q in range(2, 4):
        multiply(0, q, slice(HEAD, chunk))
        table_copy(DEPTH, q).start()
    compute(1, theirs, True)
    tail = pl.ds(HEAD, chunk - HEAD)
    remote(psend.at[0, :, :, tail], prec.at[0, :, :, tail], 0, d2d_rsem.at[0], partner).wait_recv()
    for lane in range(2):
        own[0, lane, :, HEAD:] = own[0, lane, :, HEAD:] + prec[0, lane, :, HEAD:]
        stage1_part(lane, HEAD, chunk).start()
    compute(1, ours, True)
    compute(2, theirs, True)

    def loop_send(i, carry):
        d2d_pair(i).wait_recv()
        for lane in range(2):
            own[i, lane] = own[i, lane] + prec[i, lane]
            stage1(lane, i).start()
        compute(i + 1, ours, True)
        compute(i + 2, theirs, True)
        return carry

    def loop_keep(i, carry):
        compute(i, ours, None)
        compute(i + 1, theirs, None)
        return carry

    lax.fori_loop(1, 2 * nl, loop_send, 0)
    lax.fori_loop(2 * nl + 1, steps - 1, loop_keep, 0)
    compute(steps - 1, ours, False)

    late = pl.ds(2 * nl, 2 * nl)
    remote(psend.at[late], prec.at[late], 0, d2d_rsem.at[2 * nl], partner).wait_recv()
    relay, near = pl.ds(0, nl), pl.ds(nl, nl)
    remote(own.at[relay], r1.at[relay], 1, s1_rsem.at[0], xn).wait_recv()

    def forward(j, carry):
        i = 2 * nl + j
        for lane in range(2):
            own[i, lane] = own[i, lane] + prec[i, lane] + r1[j, lane]
            stage2(lane, j).start()
        return carry

    lax.fori_loop(0, nl, forward, 0)
    remote(own.at[near], r1.at[near], 1, s1_rsem.at[1], xn).wait_recv()

    small[2].wait()
    temperature = temp[0]
    row = lax.broadcasted_iota(jnp.int32, (tokens, LANES), 0)
    lane_id = lax.broadcasted_iota(jnp.int32, (tokens, LANES), 1)
    target = jnp.zeros((tokens, LANES), jnp.int32)
    for t in range(tokens):
        target = jnp.where(row == t, tgt[t], target)
    lo = me * rows_per
    base = region_tile(me) * LANES

    def finish(j, carry):
        m, total, picked = carry
        mine_at = 3 * nl + j
        stage2_pair(j).wait_recv()
        for lane in range(2):
            z = own[mine_at, lane] + prec[mine_at, lane] + r1[nl + j, lane] + r2[j, lane]
            t = z / temperature
            off = pl.multiple_of((lane * half_tiles + j * (chunk // LANES)) * LANES, LANES)
            logits[:, pl.ds(off, chunk)] = t
            parts = []
            top = m
            for k in range(chunk // LANES):
                piece = t[:, k * LANES:(k + 1) * LANES]
                col = lane_id + (base + off + k * LANES)
                inside = (col >= lo) & (col < lo + rows_per)
                piece_in = jnp.where(inside, piece, NEG)
                picked = picked + jnp.where(inside & (col == target), piece, 0.0)
                parts.append(piece_in)
                top = jnp.maximum(top, piece_in)
            total = total * jnp.exp(m - top)
            for piece_in in parts:
                total = total + jnp.exp(piece_in - top)
            m = top
        return m, total, picked

    m, total, picked = lax.fori_loop(
        0, nl, finish,
        (jnp.full((tokens, LANES), NEG, jnp.float32), jnp.zeros((tokens, LANES), jnp.float32),
         jnp.zeros((tokens, LANES), jnp.float32)))
    m_row = jnp.max(m, axis=-1, keepdims=True)
    s_row = jnp.sum(total * jnp.exp(m - m_row), axis=-1, keepdims=True)
    p_row = jnp.sum(picked, axis=-1, keepdims=True)
    hs = tokens // 2
    lane8 = lax.broadcasted_iota(jnp.int32, (hs, LANES), 1)
    packed = jnp.broadcast_to(p_row[hs:], (hs, LANES))
    for n, v in enumerate((m_row[:hs], m_row[hs:], s_row[:hs], s_row[hs:], p_row[:hs])):
        packed = jnp.where(lane8 == n, v, packed)
    mine[...] = packed

    def share(peer):
        return remote(mine, every.at[me], 3, st_rsem.at[0], peer)

    far = me + 6 - 4 * mx - 8 * my
    peers = [far, far + 1 - 2 * core, yn, yn + 1 - 2 * core, xn, xn + 1 - 2 * core, partner]
    every[me] = packed
    for peer in peers:
        share(peer).start()

    shift = lo - base
    skip, turn = shift // LANES, shift % LANES
    rot = (LANES - turn) % LANES
    out_tiles = -(-rows_per // LANES)
    keep = lane_id < LANES - turn

    def turned(k):
        at = pl.multiple_of((skip + k) * LANES, LANES)
        return pltpu.roll(logits[:, pl.ds(at, LANES)], rot, axis=1)

    cur = turned(0)
    for k in range(out_tiles):
        if k + 1 < out_tiles:
            nxt = turned(k + 1)
        else:
            nxt = pltpu.roll(logits[:, (tiles - 1) * LANES:tiles * LANES], rot, axis=1)
        shifted[:, k * LANES:(k + 1) * LANES] = jnp.exp(jnp.where(keep, cur, nxt) - m_row)
        cur = nxt

    remote(psend, prec, 0, d2d_rsem.at[0], partner).wait_send()
    sent1 = own.at[pl.ds(0, 2 * nl)]
    remote(sent1, r1, 1, s1_rsem.at[0], xn).wait_send()
    sent2 = own.at[pl.ds(2 * nl, nl)]
    remote(sent2, r2, 2, s2_rsem.at[0], yn).wait_send()

    seven = every.at[pl.ds(0, 7)]
    remote(seven, seven, 3, st_rsem.at[0], partner).wait_recv()
    blocks_ref[...] = every[...]
    remote(seven, seven, 3, st_rsem.at[0], partner).wait_send()


def _finish_kernel(tokens, rows_per, shifted, blocks_ref, probs_hbm, ln_hbm, tl_hbm, probs, ln, tl, sem):
    row = lax.broadcasted_iota(jnp.int32, (tokens, LANES), 0)
    lane_id = lax.broadcasted_iota(jnp.int32, (tokens, LANES), 1)
    blocks = [blocks_ref[d] for d in range(8)]
    mb = blocks_ref[lax.axis_index('tp')]

    def rows16(n):
        return [jnp.concatenate([b[:, n:n + 1], b[:, n + 1:n + 2]], axis=0) for b in blocks]

    ms, ss, ps = rows16(0), rows16(2), rows16(4)
    m_all = ms[0]
    for v in ms[1:]:
        m_all = jnp.maximum(m_all, v)
    s_all = jnp.zeros_like(m_all)
    p_all = jnp.zeros_like(m_all)
    for mv, sv, pv in zip(ms, ss, ps):
        s_all = s_all + sv * jnp.exp(mv - m_all)
        p_all = p_all + pv
    log_norm = m_all + jnp.log(s_all)

    def as_row(v):
        spread = jnp.where(lane_id == row, jnp.broadcast_to(v, (tokens, LANES)), 0.0)
        return jnp.sum(spread, axis=0, keepdims=True)[:, :tokens]
    ln[...] = as_row(log_norm)
    tl[...] = as_row(p_all - log_norm)
    copies = [pltpu.make_async_copy(ln, ln_hbm, sem.at[0]), pltpu.make_async_copy(tl, tl_hbm, sem.at[1])]
    for c in copies:
        c.start()

    scale = jnp.exp(jnp.concatenate([mb[:, 0:1], mb[:, 1:2]], axis=0) - log_norm)
    step = 19 * LANES
    cut = 4 * step
    for at in range(0, rows_per, step):
        end = min(at + step, rows_per)
        probs[:, at:end] = (shifted[:, at:end] * scale).astype(jnp.bfloat16)
        if end == cut or end == rows_per:
            side = pl.ds(0, cut) if end == cut else pl.ds(cut, rows_per - cut)
            n = 2 if end == cut else 3
            copies.append(pltpu.make_async_copy(probs.at[:, side], probs_hbm.at[:, side], sem.at[n]))
            copies[-1].start()
    for c in copies:
        c.wait()


def _scores(hidden, gain, table, targets, temperature):
    tokens, hidden_dim = hidden.shape
    vocab, width = table.shape
    rows_per = vocab // 8
    nl = LANE_CHUNKS
    unit = 2 * nl
    need = -(-rows_per // LANES) + 1
    tiles = -(-need // unit) * unit
    chunk = tiles // unit * LANES
    steps = 4 * nl
    out_tiles = -(-rows_per // LANES)
    f32 = jnp.float32
    dma = pltpu.SemaphoreType.DMA
    block = (tokens, chunk)
    grows = hidden_dim // LANES
    hbm = lambda v: pltpu.with_memory_space_constraint(v, pltpu.HBM)
    shifted, blocks = pl.pallas_call(
        lambda *refs: _kernel((rows_per, tokens, width, tiles, chunk), *refs),
        out_shape=(pltpu.VMEM((tokens, out_tiles * LANES), f32), pltpu.VMEM((8, tokens // 2, LANES), f32)),
        in_specs=[pl.BlockSpec(memory_space=pltpu.HBM)] * 4 + [pl.BlockSpec(memory_space=pltpu.SMEM)],
        out_specs=(pl.BlockSpec(memory_space=pltpu.VMEM),) * 2,
        scratch_shapes=[
            pltpu.VMEM((tokens, hidden_dim), jnp.bfloat16),
            pltpu.VMEM((grows, LANES), jnp.bfloat16),
            pltpu.VMEM((grows, LANES), f32),
            pltpu.SMEM((tokens,), jnp.int32),
            pltpu.VMEM((tokens, width), jnp.bfloat16),
            pltpu.VMEM((DEPTH * 4, width, chunk), jnp.bfloat16),
            pltpu.VMEM((steps, 2) + block, f32),
            pltpu.VMEM((steps, 2) + block, f32),
            pltpu.VMEM((steps, 2) + block, f32),
            pltpu.VMEM((2 * nl, 2) + block, f32),
            pltpu.VMEM((nl, 2) + block, f32),
            pltpu.VMEM((tokens, tiles * LANES), f32),
            pltpu.VMEM((tokens // 2, LANES), f32),
            pltpu.VMEM((8, tokens // 2, LANES), f32),
            dma((3,)), dma((DEPTH * 2,)), dma((5,)),
            dma((2 * nl + 1,)), dma((2,)), dma((nl,)), dma((1,)), dma((4,)),
        ],
        compiler_params=pltpu.CompilerParams(collective_id=0, has_side_effects=True,
                                             vmem_limit_bytes=48 * 1024 * 1024),
        name='head',
    )(hbm(hidden), hbm(gain.reshape(grows, LANES)), hbm(table.T), hbm(targets), temperature.reshape(1))
    return pl.pallas_call(
        lambda *refs: _finish_kernel(tokens, rows_per, *refs),
        out_shape=(jax.ShapeDtypeStruct((tokens, rows_per), jnp.bfloat16),
                   jax.ShapeDtypeStruct((1, tokens), f32), jax.ShapeDtypeStruct((1, tokens), f32)),
        in_specs=[pl.BlockSpec(memory_space=pltpu.VMEM)] * 2,
        out_specs=(pl.BlockSpec(memory_space=pltpu.HBM),) * 3,
        scratch_shapes=[pltpu.VMEM((tokens, rows_per), jnp.bfloat16), pltpu.VMEM((1, tokens), f32),
                        pltpu.VMEM((1, tokens), f32), dma((4,))],
        compiler_params=pltpu.CompilerParams(vmem_limit_bytes=16 * 1024 * 1024),
        name='finish',
    )(shifted, blocks)


def solution(mesh):
    def local_scores(hidden, final_gain, table_cols, targets, temperature):
        probs, ln, tl = _scores(hidden, final_gain, table_cols, targets, temperature)
        return ln.reshape(-1), tl.reshape(-1), probs

    return jax.shard_map(local_scores, mesh=mesh,
                         in_specs=(P('dp', None), P(None), P(None, 'tp'), P('dp'), P()),
                         out_specs=(P('dp'), P('dp'), P('dp', 'tp')),
                         check_vma=False)
```

```python
import jax
import jax.numpy as jnp
from jax import lax
from jax.experimental import pallas as pl
from jax.experimental.pallas import tpu as pltpu
from jax.sharding import PartitionSpec as P

NORM_EPS = 1e-6
LANES = 128
LANE_CHUNKS = 3
DEPTH = 3
HEAD, MID = 4 * LANES, 11 * LANES
LAST = 5 * LANES
GROUP = 5
NEG = -3.0e38
MESH = pl.DeviceIdType.MESH


def _kernel(shape, hid_hbm, gain_hbm, table_hbm, tgt_hbm, temp, shifted, blocks_ref,
            hid, gain, gain32, tgt, normed, tbuf, psend, prec, own, r1, r2, logits, mine, every,
            in_sem, tsem, head_sem, d2d_rsem, s1_rsem, s2_rsem, st_rsem, out_sem):
    rows_per, tokens, width, tiles, chunk = shape
    half_tiles = tiles // 2
    nl = LANE_CHUNKS
    steps = 4 * nl
    me = lax.axis_index('tp')
    core, mx, my = me % 2, (me // 2) % 2, me // 4
    partner = me + 1 - 2 * core
    xn = me + 2 - 4 * mx
    yn = me + 4 - 8 * my
    first = (xn, yn)
    second = (yn, xn)

    def region_tile(d):
        return (d * rows_per) // LANES - d // 7

    def table_copy(i, q, cut=None):
        p, j = i // nl, i % nl
        lane = q % 2
        a, b = 1 - p // 2, 1 - p % 2
        fx, fy = (a, b) if lane == 0 else (b, a)
        k = 1 - core if q < 2 else core
        d = (my + fy * (1 - 2 * my)) * 4 + (mx + fx * (1 - 2 * mx)) * 2 + k
        tile = region_tile(d) + lane * half_tiles + j * (chunk // LANES)
        col = pl.multiple_of(tile * LANES, LANES)
        slot = (i % DEPTH) * 4 + q
        if cut is None:
            return pltpu.make_async_copy(table_hbm.at[:, pl.ds(col, chunk)], tbuf.at[slot],
                                         tsem.at[slot // 2])
        lo, hi, sem = cut
        return pltpu.make_async_copy(table_hbm.at[:, pl.ds(col + lo, hi - lo)],
                                     tbuf.at[slot, :, pl.ds(lo, hi - lo)], sem)

    small = [pltpu.make_async_copy(src, dst, in_sem.at[n]) for n, (src, dst) in enumerate(
        ((hid_hbm, hid), (gain_hbm, gain), (tgt_hbm, tgt)))]
    small[0].start()
    small[1].start()
    def first_copy(n):
        q = n % 4
        if n < 4:
            return table_copy(0, q, (0, HEAD, head_sem.at[min(q, 2)]))
        if n < 8:
            return table_copy(0, q, (HEAD, MID, head_sem.at[3 + q // 2]))
        return table_copy(0, q, (MID, chunk, tsem.at[q // 2]))

    for n in (0, 1, 2, 3):
        first_copy(n).start()

    barrier = pltpu.get_barrier_semaphore()
    for peer in (partner, xn, yn):
        pl.semaphore_signal(barrier, inc=1, device_id={'tp': peer}, device_id_type=MESH)

    small[0].wait()
    for n in (4, 5):
        first_copy(n).start()
    h = hid[...].astype(jnp.float32)
    inv_rms = lax.rsqrt(jnp.mean(h * h, axis=-1, keepdims=True) + NORM_EPS)
    small[1].wait()
    gain32[...] = gain[...].astype(jnp.float32)
    g0 = (me * 3) // 2
    hc = hid[:, pl.ds(pl.multiple_of(g0 * LANES, LANES), 2 * LANES)].astype(jnp.float32)
    u0 = hc[:, :LANES] * inv_rms * gain32[pl.ds(g0, 1), :]
    u1 = hc[:, LANES:] * inv_rms * gain32[pl.ds(g0 + 1, 1), :]
    u = jnp.concatenate([u0, u1], axis=1)
    u = jnp.where(core == 0, u[:, :width], u[:, 2 * LANES - width:])
    normed[...] = u.astype(jnp.bfloat16)
    for n in (6, 7, 8, 9, 10, 11):
        first_copy(n).start()

    pl.semaphore_wait(barrier, 3)

    def remote(src, dst, kind, recv, device):
        return pltpu.make_async_remote_copy(src_ref=src, dst_ref=dst, send_sem=out_sem.at[kind], recv_sem=recv,
                                            device_id={'tp': device}, device_id_type=MESH)

    def d2d(i, lane):
        return remote(psend.at[i, lane], prec.at[i, lane], 0, d2d_rsem.at[i - (i // (2 * nl)) * (i - 2 * nl)], partner)

    def d2d_part(lane, lo, hi, sem):
        at = pl.ds(lo, hi - lo)
        return remote(psend.at[0, lane, :, at], prec.at[0, lane, :, at], 0, sem, partner)

    def stage1(lane, i):
        return remote(own.at[i, lane], r1.at[i, lane], 1, s1_rsem.at[i // nl], first[lane])

    def stage1_part(lane, lo, hi):
        at = pl.ds(lo, hi - lo)
        return remote(own.at[0, lane, :, at], r1.at[0, lane, :, at], 1, s1_rsem.at[0], first[lane])

    def stage2(lane, j, lo, hi, sem):
        at = pl.ds(lo, hi - lo)
        return remote(own.at[2 * nl + j, lane, :, at], r2.at[j, lane, :, at], 2, s2_rsem.at[sem], second[lane])

    def d2d_pair(i):
        return remote(psend.at[i], prec.at[i], 0, d2d_rsem.at[i], partner)

    def stage2_pair(j, lo, hi, sem):
        at = pl.ds(lo, hi - lo)
        return remote(own.at[2 * nl + j, :, :, at], r2.at[j, :, :, at], 2, s2_rsem.at[sem], yn)

    def multiply(i, q, cols=slice(None)):
        out = psend if q < 2 else own
        slot = (i % DEPTH) * 4 + q
        out[i, q % 2, :, cols] = jnp.dot(normed[...], tbuf[slot, :, cols], preferred_element_type=jnp.float32)

    def pair_wait(i, half):
        slot = (i % DEPTH) * 4 + half * 2
        both = tbuf.at[pl.ds(slot, 2)]
        pltpu.make_async_copy(both, both, tsem.at[slot // 2]).wait()

    def compute(i, qs, prefetch):
        pair_wait(i, qs[0] // 2)
        for q in qs:
            multiply(i, q)
            if q < 2:
                d2d(i, q).start()
            if prefetch is None:
                @pl.when(i + DEPTH < steps)
                def _():
                    table_copy(i + DEPTH, q).start()
            elif prefetch:
                table_copy(i + DEPTH, q).start()

    theirs, ours = (0, 1), (2, 3)

    def piece(half, lo, hi):
        return tbuf.at[pl.ds(2 * half, 2), :, pl.ds(lo, hi - lo)]

    def landed(half, lo, hi, sem):
        pltpu.make_async_copy(piece(half, lo, hi), piece(half, lo, hi), sem).wait()

    def head_pair(lo, hi, sem):
        at = pl.ds(lo, hi - lo)
        remote(psend.at[0, :, :, at], prec.at[0, :, :, at], 0, sem, partner).wait_recv()
        for lane in range(2):
            own[0, lane, :, lo:hi] = own[0, lane, :, lo:hi] + prec[0, lane, :, lo:hi]
            stage1_part(lane, lo, hi).start()

    for q in range(2):
        first_copy(q).wait()
        multiply(0, q, slice(0, HEAD))
        d2d_part(q, 0, HEAD, head_sem.at[5 + q]).start()
    landed(1, 0, HEAD, head_sem.at[2])
    for q in range(2, 4):
        multiply(0, q, slice(0, HEAD))
    landed(0, HEAD, MID, head_sem.at[3])
    for q in range(2):
        multiply(0, q, slice(HEAD, MID))
        d2d_part(q, HEAD, MID, head_sem.at[7]).start()
    for q in range(4):
        table_copy(1, q).start()
    for lane in range(2):
        d2d_part(lane, 0, HEAD, head_sem.at[5 + lane]).wait_recv()
        own[0, lane, :, :HEAD] = own[0, lane, :, :HEAD] + prec[0, lane, :, :HEAD]
        stage1_part(lane, 0, HEAD).start()
    landed(0, MID, chunk, tsem.at[0])
    for q in range(2):
        multiply(0, q, slice(MID, chunk))
        d2d_part(q, MID, chunk, d2d_rsem.at[0]).start()
    landed(1, HEAD, MID, head_sem.at[4])
    for q in range(2, 4):
        multiply(0, q, slice(HEAD, MID))
    head_pair(HEAD, MID, head_sem.at[7])
    for i in range(2, DEPTH):
        for q in range(4):
            table_copy(i, q).start()
    landed(1, MID, chunk, tsem.at[1])
    for q in range(2, 4):
        multiply(0, q, slice(MID, chunk))
    for q in range(4):
        table_copy(DEPTH, q).start()
    small[2].start()
    head_pair(MID, chunk, d2d_rsem.at[0])
    compute(1, theirs, True)
    compute(1, ours, True)
    compute(2, theirs, True)

    def loop_send(i, carry):
        d2d_pair(i).wait_recv()
        for lane in range(2):
            own[i, lane] = own[i, lane] + prec[i, lane]
            stage1(lane, i).start()
        compute(i + 1, ours, True)
        compute(i + 2, theirs, True)
        return carry

    def loop_keep(i, carry):
        compute(i, ours, None)
        compute(i + 1, theirs, None)
        return carry

    lax.fori_loop(1, 2 * nl, loop_send, 0)
    lax.fori_loop(2 * nl + 1, steps - 1, loop_keep, 0)
    compute(steps - 1, ours, False)

    late = pl.ds(2 * nl, 2 * nl)
    remote(psend.at[late], prec.at[late], 0, d2d_rsem.at[2 * nl], partner).wait_recv()
    relay, near = pl.ds(0, nl), pl.ds(nl, nl)
    remote(own.at[relay], r1.at[relay], 1, s1_rsem.at[0], xn).wait_recv()

    pieces = [(j, 0, chunk) for j in range(nl - 1)] + [(nl - 1, 0, chunk - LAST), (nl - 1, chunk - LAST, chunk)]

    for n, (j, lo, hi) in enumerate(pieces):
        i = 2 * nl + j
        for lane in range(2):
            own[i, lane, :, lo:hi] = own[i, lane, :, lo:hi] + prec[i, lane, :, lo:hi] + r1[j, lane, :, lo:hi]
            stage2(lane, j, lo, hi, n).start()

    remote(own.at[near], r1.at[near], 1, s1_rsem.at[1], xn).wait_recv()

    small[2].wait()
    inv_temp = 1.0 / jnp.full((tokens, LANES), temp[0], jnp.float32)
    row = lax.broadcasted_iota(jnp.int32, (tokens, LANES), 0)
    lane_id = lax.broadcasted_iota(jnp.int32, (tokens, LANES), 1)
    target = jnp.zeros((tokens, LANES), jnp.int32)
    for t in range(tokens):
        target = jnp.where(row == t, tgt[t], target)
    lo_row = me * rows_per
    shift = lo_row - region_tile(me) * LANES
    rel = target - lo_row
    rel = jnp.where((rel >= 0) & (rel < rows_per), rel + shift, -1)
    edge = (0, 1, tiles - 2, tiles - 1)

    m = jnp.full((tokens, LANES), NEG, jnp.float32)
    total = jnp.zeros((tokens, LANES), jnp.float32)
    picked = jnp.zeros((tokens, LANES), jnp.float32)
    for n, (j, lo, hi) in enumerate(pieces):
        i = 3 * nl + j
        stage2_pair(j, lo, hi, n).wait_recv()
        for lane in range(2):
            for at in range(lo, hi, GROUP * LANES):
                parts = []
                top = m
                for k in range(GROUP):
                    c = slice(at + k * LANES, at + (k + 1) * LANES)
                    tile = lane * half_tiles + j * (chunk // LANES) + at // LANES + k
                    z = own[i, lane, :, c] + prec[i, lane, :, c] + r1[nl + j, lane, :, c] + r2[j, lane, :, c]
                    t = z * inv_temp
                    logits[:, tile * LANES:(tile + 1) * LANES] = t
                    picked = picked + jnp.where(lane_id == rel - tile * LANES, t, 0.0)
                    if tile in edge:
                        col = lane_id + (tile * LANES - shift)
                        t = jnp.where((col >= 0) & (col < rows_per), t, NEG)
                    parts.append(t)
                    top = jnp.maximum(top, t)
                total = total * jnp.exp(m - top)
                for t in parts:
                    total = total + jnp.exp(t - top)
                m = top
    m_row = jnp.max(m, axis=-1, keepdims=True)
    s_row = jnp.sum(total * jnp.exp(m - m_row), axis=-1, keepdims=True)
    p_row = jnp.sum(picked, axis=-1, keepdims=True)
    hs = tokens // 2
    lane8 = lax.broadcasted_iota(jnp.int32, (hs, LANES), 1)
    mine[0] = jnp.where(lane8 < 64, jnp.where(lane8 < 32, m_row[:hs], m_row[hs:]),
                        jnp.where(lane8 < 96, p_row[:hs], p_row[hs:]))
    mine[1] = jnp.where(lane8 < 32, s_row[:hs], s_row[hs:])

    def share(peer):
        return remote(mine, every.at[me], 3, st_rsem.at[0], peer)

    far = me + 6 - 4 * mx - 8 * my
    peers = [far, far + 1 - 2 * core, yn, yn + 1 - 2 * core, xn, xn + 1 - 2 * core, partner]
    every[me] = mine[...]
    for peer in peers:
        share(peer).start()

    skip, turn = shift // LANES, shift % LANES
    rot = (LANES - turn) % LANES
    out_tiles = -(-rows_per // LANES)
    keep = lane_id < LANES - turn

    def turned(k):
        at = pl.multiple_of((skip + k) * LANES, LANES)
        return pltpu.roll(logits[:, pl.ds(at, LANES)], rot, axis=1)

    cur = turned(0)
    for k in range(out_tiles):
        if k + 1 < out_tiles:
            nxt = turned(k + 1)
        else:
            nxt = pltpu.roll(logits[:, (tiles - 1) * LANES:tiles * LANES], rot, axis=1)
        shifted[:, k * LANES:(k + 1) * LANES] = jnp.exp(jnp.where(keep, cur, nxt) - m_row)
        cur = nxt

    remote(psend, prec, 0, d2d_rsem.at[0], partner).wait_send()
    sent1 = own.at[pl.ds(0, 2 * nl)]
    remote(sent1, r1, 1, s1_rsem.at[0], xn).wait_send()
    sent2 = own.at[pl.ds(2 * nl, nl)]
    remote(sent2, r2, 2, s2_rsem.at[0], yn).wait_send()

    seven = every.at[pl.ds(0, 7)]
    remote(seven, seven, 3, st_rsem.at[0], partner).wait_recv()
    blocks_ref[...] = every[...]
    remote(seven, seven, 3, st_rsem.at[0], partner).wait_send()


def _finish_kernel(tokens, rows_per, shifted, blocks_ref, probs_hbm, ln_hbm, tl_hbm, probs, ln, tl, sem):
    row = lax.broadcasted_iota(jnp.int32, (tokens, LANES), 0)
    lane_id = lax.broadcasted_iota(jnp.int32, (tokens, LANES), 1)
    def tree(op, vs):
        while len(vs) > 1:
            vs = [op(vs[k], vs[k + 1]) for k in range(0, len(vs), 2)]
        return vs[0]

    def rows16(v, at):
        return jnp.concatenate([v[:, at:at + 1], v[:, at + 32:at + 33]], axis=0)

    tops = [blocks_ref[d, 0] for d in range(8)]
    m_all = tree(jnp.maximum, tops)
    s_all = tree(jnp.add, [blocks_ref[d, 1] * jnp.exp(tops[d] - m_all) for d in range(8)])
    log_all = m_all + jnp.log(s_all)
    scale = rows16(jnp.exp(blocks_ref[lax.axis_index('tp'), 0] - log_all), 0)
    log_norm = rows16(log_all, 0)
    p_all = rows16(tree(jnp.add, tops), 64)

    def as_row(v):
        spread = jnp.where(lane_id == row, jnp.broadcast_to(v, (tokens, LANES)), 0.0)
        return jnp.sum(spread, axis=0, keepdims=True)[:, :tokens]

    cut = 76 * LANES
    sides = (pl.ds(0, cut), pl.ds(cut, rows_per - cut))
    copies = [pltpu.make_async_copy(probs.at[:, side], probs_hbm.at[:, side], sem.at[n]) for n, side in enumerate(sides)]
    copies += [pltpu.make_async_copy(ln, ln_hbm, sem.at[2]), pltpu.make_async_copy(tl, tl_hbm, sem.at[3])]
    probs[:, :cut] = (shifted[:, :cut] * scale).astype(jnp.bfloat16)
    copies[0].start()
    ln[...] = as_row(log_norm)
    tl[...] = as_row(p_all - log_norm)
    probs[:, cut:rows_per] = (shifted[:, cut:rows_per] * scale).astype(jnp.bfloat16)
    for c in copies[1:]:
        c.start()
    for c in copies:
        c.wait()


def _scores(hidden, gain, table, targets, temperature):
    tokens, hidden_dim = hidden.shape
    vocab, width = table.shape
    rows_per = vocab // 8
    nl = LANE_CHUNKS
    unit = 2 * nl
    need = -(-rows_per // LANES) + 1
    tiles = -(-need // unit) * unit
    chunk = tiles // unit * LANES
    steps = 4 * nl
    out_tiles = -(-rows_per // LANES)
    f32 = jnp.float32
    dma = pltpu.SemaphoreType.DMA
    block = (tokens, chunk)
    grows = hidden_dim // LANES
    hbm = lambda v: pltpu.with_memory_space_constraint(v, pltpu.HBM)
    shifted, blocks = pl.pallas_call(
        lambda *refs: _kernel((rows_per, tokens, width, tiles, chunk), *refs),
        out_shape=(pltpu.VMEM((tokens, out_tiles * LANES), f32), pltpu.VMEM((8, 2, tokens // 2, LANES), f32)),
        in_specs=[pl.BlockSpec(memory_space=pltpu.HBM)] * 4 + [pl.BlockSpec(memory_space=pltpu.SMEM)],
        out_specs=(pl.BlockSpec(memory_space=pltpu.VMEM),) * 2,
        scratch_shapes=[
            pltpu.VMEM((tokens, hidden_dim), jnp.bfloat16),
            pltpu.VMEM((grows, LANES), jnp.bfloat16),
            pltpu.VMEM((grows, LANES), f32),
            pltpu.SMEM((tokens,), jnp.int32),
            pltpu.VMEM((tokens, width), jnp.bfloat16),
            pltpu.VMEM((DEPTH * 4, width, chunk), jnp.bfloat16),
            pltpu.VMEM((steps, 2) + block, f32),
            pltpu.VMEM((steps, 2) + block, f32),
            pltpu.VMEM((steps, 2) + block, f32),
            pltpu.VMEM((2 * nl, 2) + block, f32),
            pltpu.VMEM((nl, 2) + block, f32),
            pltpu.VMEM((tokens, tiles * LANES), f32),
            pltpu.VMEM((2, tokens // 2, LANES), f32),
            pltpu.VMEM((8, 2, tokens // 2, LANES), f32),
            dma((3,)), dma((DEPTH * 2,)), dma((8,)),
            dma((2 * nl + 1,)), dma((2,)), dma((nl + 1,)), dma((1,)), dma((4,)),
        ],
        compiler_params=pltpu.CompilerParams(collective_id=0, has_side_effects=True,
                                             vmem_limit_bytes=48 * 1024 * 1024),
        name='head',
    )(hbm(hidden), hbm(gain.reshape(grows, LANES)), hbm(table.T), hbm(targets), temperature.reshape(1))
    return pl.pallas_call(
        lambda *refs: _finish_kernel(tokens, rows_per, *refs),
        out_shape=(jax.ShapeDtypeStruct((tokens, rows_per), jnp.bfloat16),
                   jax.ShapeDtypeStruct((1, tokens), f32), jax.ShapeDtypeStruct((1, tokens), f32)),
        in_specs=[pl.BlockSpec(memory_space=pltpu.VMEM)] * 2,
        out_specs=(pl.BlockSpec(memory_space=pltpu.HBM),) * 3,
        scratch_shapes=[pltpu.VMEM((tokens, rows_per), jnp.bfloat16), pltpu.VMEM((1, tokens), f32),
                        pltpu.VMEM((1, tokens), f32), dma((4,))],
        compiler_params=pltpu.CompilerParams(vmem_limit_bytes=16 * 1024 * 1024),
        name='finish',
    )(shifted, blocks)


def solution(mesh):
    def local_scores(hidden, final_gain, table_cols, targets, temperature):
        probs, ln, tl = _scores(hidden, final_gain, table_cols, targets, temperature)
        return ln.reshape(-1), tl.reshape(-1), probs

    return jax.shard_map(local_scores, mesh=mesh,
                         in_specs=(P('dp', None), P(None), P(None, 'tp'), P('dp'), P()),
                         out_specs=(P('dp'), P('dp'), P('dp', 'tp')),
                         check_vma=False)
```

```python
import jax
import jax.numpy as jnp
from jax import lax
from jax.experimental import pallas as pl
from jax.experimental.pallas import tpu as pltpu
from jax.sharding import PartitionSpec as P

NORM_EPS = 1e-6
LANES = 128
LANE_CHUNKS = 3
DEPTH = 3
HEAD, MID = 4 * LANES, 11 * LANES
LAST = 5 * LANES
GROUP = 5
NEG = -3.0e38
MESH = pl.DeviceIdType.MESH


def _kernel(shape, hid_hbm, gain_hbm, table_hbm, tgt_hbm, temp, shifted, blocks_ref,
            hid, gain, gain32, tgt, normed, tbuf, psend, prec, own, r1, r2, logits, mine, every,
            in_sem, tsem, head_sem, d2d_rsem, s1_rsem, s2_rsem, st_rsem, out_sem):
    rows_per, tokens, width, tiles, chunk = shape
    half_tiles = tiles // 2
    nl = LANE_CHUNKS
    steps = 4 * nl
    me = lax.axis_index('tp')
    core, mx, my = me % 2, (me // 2) % 2, me // 4
    partner = me + 1 - 2 * core
    xn = me + 2 - 4 * mx
    yn = me + 4 - 8 * my
    first = (xn, yn)
    second = (yn, xn)

    def region_tile(d):
        return (d * rows_per) // LANES - d // 7

    def table_copy(i, q, cut=None):
        p, j = i // nl, i % nl
        lane = q % 2
        a, b = 1 - p // 2, 1 - p % 2
        fx, fy = (a, b) if lane == 0 else (b, a)
        k = 1 - core if q < 2 else core
        d = (my + fy * (1 - 2 * my)) * 4 + (mx + fx * (1 - 2 * mx)) * 2 + k
        tile = region_tile(d) + lane * half_tiles + j * (chunk // LANES)
        col = pl.multiple_of(tile * LANES, LANES)
        slot = (i % DEPTH) * 4 + q
        if cut is None:
            return pltpu.make_async_copy(table_hbm.at[:, pl.ds(col, chunk)], tbuf.at[slot],
                                         tsem.at[slot // 2])
        lo, hi, sem = cut
        return pltpu.make_async_copy(table_hbm.at[:, pl.ds(col + lo, hi - lo)],
                                     tbuf.at[slot, :, pl.ds(lo, hi - lo)], sem)

    small = [pltpu.make_async_copy(src, dst, in_sem.at[n]) for n, (src, dst) in enumerate(
        ((hid_hbm, hid), (gain_hbm, gain), (tgt_hbm, tgt)))]
    small[0].start()
    small[1].start()
    def first_copy(n):
        q = n % 4
        if n < 4:
            return table_copy(0, q, (0, HEAD, head_sem.at[min(q, 2)]))
        if n < 8:
            return table_copy(0, q, (HEAD, MID, head_sem.at[3 + q // 2]))
        return table_copy(0, q, (MID, chunk, tsem.at[q // 2]))

    for n in (0, 1, 2, 3, 4, 5):
        first_copy(n).start()

    barrier = pltpu.get_barrier_semaphore()
    for peer in (partner, xn, yn):
        pl.semaphore_signal(barrier, inc=1, device_id={'tp': peer}, device_id_type=MESH)

    small[0].wait()
    for n in (6, 7, 8, 9, 10, 11):
        first_copy(n).start()
    h = hid[...].astype(jnp.float32)
    inv_rms = lax.rsqrt(jnp.mean(h * h, axis=-1, keepdims=True) + NORM_EPS)
    small[1].wait()
    gain32[...] = gain[...].astype(jnp.float32)
    g0 = (me * 3) // 2
    hc = hid[:, pl.ds(pl.multiple_of(g0 * LANES, LANES), 2 * LANES)].astype(jnp.float32)
    u0 = hc[:, :LANES] * inv_rms * gain32[pl.ds(g0, 1), :]
    u1 = hc[:, LANES:] * inv_rms * gain32[pl.ds(g0 + 1, 1), :]
    u = jnp.concatenate([u0, u1], axis=1)
    u = jnp.where(core == 0, u[:, :width], u[:, 2 * LANES - width:])
    normed[...] = u.astype(jnp.bfloat16)

    pl.semaphore_wait(barrier, 3)

    def remote(src, dst, kind, recv, device):
        return pltpu.make_async_remote_copy(src_ref=src, dst_ref=dst, send_sem=out_sem.at[kind], recv_sem=recv,
                                            device_id={'tp': device}, device_id_type=MESH)

    def d2d(i, lane):
        return remote(psend.at[i, lane], prec.at[i, lane], 0, d2d_rsem.at[i - (i // (2 * nl)) * (i - 2 * nl)], partner)

    def d2d_part(lane, lo, hi, sem):
        at = pl.ds(lo, hi - lo)
        return remote(psend.at[0, lane, :, at], prec.at[0, lane, :, at], 0, sem, partner)

    def stage1(lane, i):
        return remote(own.at[i, lane], r1.at[i, lane], 1, s1_rsem.at[i // nl], first[lane])

    def stage1_part(lane, lo, hi):
        at = pl.ds(lo, hi - lo)
        return remote(own.at[0, lane, :, at], r1.at[0, lane, :, at], 1, s1_rsem.at[0], first[lane])

    def stage2(lane, j, lo, hi, sem):
        at = pl.ds(lo, hi - lo)
        return remote(own.at[2 * nl + j, lane, :, at], r2.at[j, lane, :, at], 2, s2_rsem.at[sem], second[lane])

    def d2d_pair(i):
        return remote(psend.at[i], prec.at[i], 0, d2d_rsem.at[i], partner)

    def stage2_pair(j, lo, hi, sem):
        at = pl.ds(lo, hi - lo)
        return remote(own.at[2 * nl + j, :, :, at], r2.at[j, :, :, at], 2, s2_rsem.at[sem], yn)

    def multiply(i, q, cols=slice(None)):
        out = psend if q < 2 else own
        slot = (i % DEPTH) * 4 + q
        out[i, q % 2, :, cols] = jnp.dot(normed[...], tbuf[slot, :, cols], preferred_element_type=jnp.float32)

    def pair_wait(i, half):
        slot = (i % DEPTH) * 4 + half * 2
        both = tbuf.at[pl.ds(slot, 2)]
        pltpu.make_async_copy(both, both, tsem.at[slot // 2]).wait()

    def compute(i, qs, prefetch):
        pair_wait(i, qs[0] // 2)
        for q in qs:
            multiply(i, q)
            if q < 2:
                d2d(i, q).start()
            if prefetch is None:
                @pl.when(i + DEPTH < steps)
                def _():
                    table_copy(i + DEPTH, q).start()
            elif prefetch:
                table_copy(i + DEPTH, q).start()

    theirs, ours = (0, 1), (2, 3)

    def piece(half, lo, hi):
        return tbuf.at[pl.ds(2 * half, 2), :, pl.ds(lo, hi - lo)]

    def landed(half, lo, hi, sem):
        pltpu.make_async_copy(piece(half, lo, hi), piece(half, lo, hi), sem).wait()

    def head_pair(lo, hi, sem):
        at = pl.ds(lo, hi - lo)
        remote(psend.at[0, :, :, at], prec.at[0, :, :, at], 0, sem, partner).wait_recv()
        for lane in range(2):
            own[0, lane, :, lo:hi] = own[0, lane, :, lo:hi] + prec[0, lane, :, lo:hi]
            stage1_part(lane, lo, hi).start()

    for q in range(2):
        first_copy(q).wait()
        multiply(0, q, slice(0, HEAD))
        d2d_part(q, 0, HEAD, head_sem.at[5 + q]).start()
    landed(1, 0, HEAD, head_sem.at[2])
    for q in range(2, 4):
        multiply(0, q, slice(0, HEAD))
    landed(0, HEAD, MID, head_sem.at[3])
    for q in range(2):
        multiply(0, q, slice(HEAD, MID))
        d2d_part(q, HEAD, MID, head_sem.at[7]).start()
    for q in range(4):
        table_copy(1, q).start()
    for lane in range(2):
        d2d_part(lane, 0, HEAD, head_sem.at[5 + lane]).wait_recv()
        own[0, lane, :, :HEAD] = own[0, lane, :, :HEAD] + prec[0, lane, :, :HEAD]
        stage1_part(lane, 0, HEAD).start()
    landed(0, MID, chunk, tsem.at[0])
    for q in range(2):
        multiply(0, q, slice(MID, chunk))
        d2d_part(q, MID, chunk, d2d_rsem.at[0]).start()
    landed(1, HEAD, MID, head_sem.at[4])
    for q in range(2, 4):
        multiply(0, q, slice(HEAD, MID))
    head_pair(HEAD, MID, head_sem.at[7])
    for i in range(2, DEPTH):
        for q in range(4):
            table_copy(i, q).start()
    landed(1, MID, chunk, tsem.at[1])
    for q in range(2, 4):
        multiply(0, q, slice(MID, chunk))
    for q in range(4):
        table_copy(DEPTH, q).start()
    small[2].start()
    head_pair(MID, chunk, d2d_rsem.at[0])
    compute(1, theirs, True)
    compute(1, ours, True)
    compute(2, theirs, True)

    def loop_send(i, carry):
        d2d_pair(i).wait_recv()
        for lane in range(2):
            own[i, lane] = own[i, lane] + prec[i, lane]
            stage1(lane, i).start()
        compute(i + 1, ours, True)
        compute(i + 2, theirs, True)
        return carry

    def loop_keep(i, carry):
        compute(i, ours, None)
        compute(i + 1, theirs, None)
        return carry

    lax.fori_loop(1, 2 * nl, loop_send, 0)
    lax.fori_loop(2 * nl + 1, steps - 1, loop_keep, 0)
    compute(steps - 1, ours, False)

    late = pl.ds(2 * nl, 2 * nl)
    remote(psend.at[late], prec.at[late], 0, d2d_rsem.at[2 * nl], partner).wait_recv()
    relay, near = pl.ds(0, nl), pl.ds(nl, nl)
    remote(own.at[relay], r1.at[relay], 1, s1_rsem.at[0], xn).wait_recv()

    pieces = [(j, 0, chunk) for j in range(nl - 1)] + [(nl - 1, 0, chunk - LAST), (nl - 1, chunk - LAST, chunk)]

    def first_sent():
        remote(own.at[pl.ds(0, 2 * nl)], r1, 1, s1_rsem.at[0], xn).wait_send()

    @pl.when(core == 1)
    def _():
        first_sent()

    for n, (j, lo, hi) in enumerate(pieces):
        i = 2 * nl + j
        if n in (1, 2):
            @pl.when(core == 1)
            def _():
                pj, plo, phi = pieces[n - 1]
                stage2_pair(pj, plo, phi, n - 1).wait_send()
        for lane in range(2):
            own[i, lane, :, lo:hi] = own[i, lane, :, lo:hi] + prec[i, lane, :, lo:hi] + r1[j, lane, :, lo:hi]
            stage2(lane, j, lo, hi, n).start()

    remote(own.at[near], r1.at[near], 1, s1_rsem.at[1], xn).wait_recv()

    small[2].wait()
    inv_temp = 1.0 / jnp.full((tokens, LANES), temp[0], jnp.float32)
    row = lax.broadcasted_iota(jnp.int32, (tokens, LANES), 0)
    lane_id = lax.broadcasted_iota(jnp.int32, (tokens, LANES), 1)
    target = jnp.zeros((tokens, LANES), jnp.int32)
    for t in range(tokens):
        target = jnp.where(row == t, tgt[t], target)
    lo_row = me * rows_per
    shift = lo_row - region_tile(me) * LANES
    rel = target - lo_row
    rel = jnp.where((rel >= 0) & (rel < rows_per), rel + shift, -1)
    edge = (0, 1, tiles - 2, tiles - 1)

    m = jnp.full((tokens, LANES), NEG, jnp.float32)
    total = jnp.zeros((tokens, LANES), jnp.float32)
    picked = jnp.zeros((tokens, LANES), jnp.float32)
    for n, (j, lo, hi) in enumerate(pieces):
        i = 3 * nl + j
        stage2_pair(j, lo, hi, n).wait_recv()
        for lane in range(2):
            for at in range(lo, hi, GROUP * LANES):
                parts = []
                top = m
                for k in range(GROUP):
                    c = slice(at + k * LANES, at + (k + 1) * LANES)
                    tile = lane * half_tiles + j * (chunk // LANES) + at // LANES + k
                    z = own[i, lane, :, c] + prec[i, lane, :, c] + r1[nl + j, lane, :, c] + r2[j, lane, :, c]
                    t = z * inv_temp
                    logits[:, tile * LANES:(tile + 1) * LANES] = t
                    picked = picked + jnp.where(lane_id == rel - tile * LANES, t, 0.0)
                    if tile in edge:
                        col = lane_id + (tile * LANES - shift)
                        t = jnp.where((col >= 0) & (col < rows_per), t, NEG)
                    parts.append(t)
                    top = jnp.maximum(top, t)
                total = total * jnp.exp(m - top)
                for t in parts:
                    total = total + jnp.exp(t - top)
                m = top
    m_row = jnp.max(m, axis=-1, keepdims=True)
    s_row = jnp.sum(total * jnp.exp(m - m_row), axis=-1, keepdims=True)
    p_row = jnp.sum(picked, axis=-1, keepdims=True)
    hs = tokens // 2
    lane8 = lax.broadcasted_iota(jnp.int32, (hs, LANES), 1)
    mine[0] = jnp.where(lane8 < 64, jnp.where(lane8 < 32, m_row[:hs], m_row[hs:]),
                        jnp.where(lane8 < 96, p_row[:hs], p_row[hs:]))
    mine[1] = jnp.where(lane8 < 32, s_row[:hs], s_row[hs:])

    def share(peer):
        return remote(mine, every.at[me], 3, st_rsem.at[0], peer)

    far = me + 6 - 4 * mx - 8 * my
    peers = [far, far + 1 - 2 * core, yn, yn + 1 - 2 * core, xn, xn + 1 - 2 * core, partner]
    every[me] = mine[...]
    for peer in peers:
        share(peer).start()

    skip, turn = shift // LANES, shift % LANES
    rot = (LANES - turn) % LANES
    out_tiles = -(-rows_per // LANES)
    keep = lane_id < LANES - turn

    def turned(k):
        at = pl.multiple_of((skip + k) * LANES, LANES)
        return pltpu.roll(logits[:, pl.ds(at, LANES)], rot, axis=1)

    cur = turned(0)
    for k in range(out_tiles):
        if k + 1 < out_tiles:
            nxt = turned(k + 1)
        else:
            nxt = pltpu.roll(logits[:, (tiles - 1) * LANES:tiles * LANES], rot, axis=1)
        shifted[:, k * LANES:(k + 1) * LANES] = jnp.exp(jnp.where(keep, cur, nxt) - m_row)
        cur = nxt

    remote(psend, prec, 0, d2d_rsem.at[0], partner).wait_send()
    @pl.when(core == 0)
    def _():
        first_sent()
    for n, (j, lo, hi) in enumerate(pieces):
        if n + 1 in (1, 2):
            @pl.when(core == 0)
            def _():
                stage2_pair(j, lo, hi, n).wait_send()
        else:
            stage2_pair(j, lo, hi, n).wait_send()

    seven = every.at[pl.ds(0, 7)]
    remote(seven, seven, 3, st_rsem.at[0], partner).wait_recv()
    blocks_ref[...] = every[...]
    remote(seven, seven, 3, st_rsem.at[0], partner).wait_send()


def _finish_kernel(tokens, rows_per, shifted, blocks_ref, probs_hbm, ln_hbm, tl_hbm, probs, ln, tl, sem):
    row = lax.broadcasted_iota(jnp.int32, (tokens, LANES), 0)
    lane_id = lax.broadcasted_iota(jnp.int32, (tokens, LANES), 1)
    def tree(op, vs):
        while len(vs) > 1:
            vs = [op(vs[k], vs[k + 1]) for k in range(0, len(vs), 2)]
        return vs[0]

    def rows16(v, at):
        return jnp.concatenate([v[:, at:at + 1], v[:, at + 32:at + 33]], axis=0)

    tops = [blocks_ref[d, 0] for d in range(8)]
    m_all = tree(jnp.maximum, tops)
    s_all = tree(jnp.add, [blocks_ref[d, 1] * jnp.exp(tops[d] - m_all) for d in range(8)])
    log_all = m_all + jnp.log(s_all)
    scale = rows16(jnp.exp(blocks_ref[lax.axis_index('tp'), 0] - log_all), 0)
    log_norm = rows16(log_all, 0)
    p_all = rows16(tree(jnp.add, tops), 64)

    def as_row(v):
        spread = jnp.where(lane_id == row, jnp.broadcast_to(v, (tokens, LANES)), 0.0)
        return jnp.sum(spread, axis=0, keepdims=True)[:, :tokens]

    cut = 76 * LANES
    sides = (pl.ds(0, cut), pl.ds(cut, rows_per - cut))
    copies = [pltpu.make_async_copy(probs.at[:, side], probs_hbm.at[:, side], sem.at[n]) for n, side in enumerate(sides)]
    copies += [pltpu.make_async_copy(ln, ln_hbm, sem.at[2]), pltpu.make_async_copy(tl, tl_hbm, sem.at[3])]
    probs[:, :cut] = (shifted[:, :cut] * scale).astype(jnp.bfloat16)
    copies[0].start()
    ln[...] = as_row(log_norm)
    tl[...] = as_row(p_all - log_norm)
    probs[:, cut:rows_per] = (shifted[:, cut:rows_per] * scale).astype(jnp.bfloat16)
    for c in copies[1:]:
        c.start()
    for c in copies:
        c.wait()


def _scores(hidden, gain, table, targets, temperature):
    tokens, hidden_dim = hidden.shape
    vocab, width = table.shape
    rows_per = vocab // 8
    nl = LANE_CHUNKS
    unit = 2 * nl
    need = -(-rows_per // LANES) + 1
    tiles = -(-need // unit) * unit
    chunk = tiles // unit * LANES
    steps = 4 * nl
    out_tiles = -(-rows_per // LANES)
    f32 = jnp.float32
    dma = pltpu.SemaphoreType.DMA
    block = (tokens, chunk)
    grows = hidden_dim // LANES
    hbm = lambda v: pltpu.with_memory_space_constraint(v, pltpu.HBM)
    shifted, blocks = pl.pallas_call(
        lambda *refs: _kernel((rows_per, tokens, width, tiles, chunk), *refs),
        out_shape=(pltpu.VMEM((tokens, out_tiles * LANES), f32), pltpu.VMEM((8, 2, tokens // 2, LANES), f32)),
        in_specs=[pl.BlockSpec(memory_space=pltpu.HBM)] * 4 + [pl.BlockSpec(memory_space=pltpu.SMEM)],
        out_specs=(pl.BlockSpec(memory_space=pltpu.VMEM),) * 2,
        scratch_shapes=[
            pltpu.VMEM((tokens, hidden_dim), jnp.bfloat16),
            pltpu.VMEM((grows, LANES), jnp.bfloat16),
            pltpu.VMEM((grows, LANES), f32),
            pltpu.SMEM((tokens,), jnp.int32),
            pltpu.VMEM((tokens, width), jnp.bfloat16),
            pltpu.VMEM((DEPTH * 4, width, chunk), jnp.bfloat16),
            pltpu.VMEM((steps, 2) + block, f32),
            pltpu.VMEM((steps, 2) + block, f32),
            pltpu.VMEM((steps, 2) + block, f32),
            pltpu.VMEM((2 * nl, 2) + block, f32),
            pltpu.VMEM((nl, 2) + block, f32),
            pltpu.VMEM((tokens, tiles * LANES), f32),
            pltpu.VMEM((2, tokens // 2, LANES), f32),
            pltpu.VMEM((8, 2, tokens // 2, LANES), f32),
            dma((3,)), dma((DEPTH * 2,)), dma((8,)),
            dma((2 * nl + 1,)), dma((2,)), dma((nl + 1,)), dma((1,)), dma((4,)),
        ],
        compiler_params=pltpu.CompilerParams(collective_id=0, has_side_effects=True,
                                             vmem_limit_bytes=48 * 1024 * 1024),
        name='head',
    )(hbm(hidden), hbm(gain.reshape(grows, LANES)), hbm(table.T), hbm(targets), temperature.reshape(1))
    return pl.pallas_call(
        lambda *refs: _finish_kernel(tokens, rows_per, *refs),
        out_shape=(jax.ShapeDtypeStruct((tokens, rows_per), jnp.bfloat16),
                   jax.ShapeDtypeStruct((1, tokens), f32), jax.ShapeDtypeStruct((1, tokens), f32)),
        in_specs=[pl.BlockSpec(memory_space=pltpu.VMEM)] * 2,
        out_specs=(pl.BlockSpec(memory_space=pltpu.HBM),) * 3,
        scratch_shapes=[pltpu.VMEM((tokens, rows_per), jnp.bfloat16), pltpu.VMEM((1, tokens), f32),
                        pltpu.VMEM((1, tokens), f32), dma((4,))],
        compiler_params=pltpu.CompilerParams(vmem_limit_bytes=16 * 1024 * 1024),
        name='finish',
    )(shifted, blocks)


def solution(mesh):
    def local_scores(hidden, final_gain, table_cols, targets, temperature):
        probs, ln, tl = _scores(hidden, final_gain, table_cols, targets, temperature)
        return ln.reshape(-1), tl.reshape(-1), probs

    return jax.shard_map(local_scores, mesh=mesh,
                         in_specs=(P('dp', None), P(None), P(None, 'tp'), P('dp'), P()),
                         out_specs=(P('dp'), P('dp'), P('dp', 'tp')),
                         check_vma=False)
```

```python
import jax
import jax.numpy as jnp
from jax import lax
from jax.experimental import pallas as pl
from jax.experimental.pallas import tpu as pltpu
from jax.sharding import PartitionSpec as P

NORM_EPS = 1e-6
LANES = 128
LANE_CHUNKS = 3
DEPTH = 2
HEAD, MID = 4 * LANES, 11 * LANES
LAST = 5 * LANES
GROUP = 5
NEG = -3.0e38
MESH = pl.DeviceIdType.MESH


def _kernel(shape, hid_hbm, gain_hbm, table_hbm, tgt_hbm, temp, shifted, blocks_ref,
            hid, gain, gain32, tgt, normed, tbuf, psend, prec, own, r1, r2, logits, mine, every,
            in_sem, tsem, head_sem, d2d_rsem, s1_rsem, s2_rsem, st_rsem, out_sem):
    rows_per, tokens, width, tiles, chunk = shape
    half_tiles = tiles // 2
    nl = LANE_CHUNKS
    steps = 4 * nl
    me = lax.axis_index('tp')
    core, mx, my = me % 2, (me // 2) % 2, me // 4
    partner = me + 1 - 2 * core
    xn = me + 2 - 4 * mx
    yn = me + 4 - 8 * my
    first = (xn, yn)
    second = (yn, xn)

    def region_tile(d):
        return (d * rows_per) // LANES - d // 7

    def table_copy(i, q, cut=None):
        p, j = i // nl, i % nl
        lane = q % 2
        a, b = 1 - p // 2, 1 - p % 2
        fx, fy = (a, b) if lane == 0 else (b, a)
        k = 1 - core if q < 2 else core
        d = (my + fy * (1 - 2 * my)) * 4 + (mx + fx * (1 - 2 * mx)) * 2 + k
        tile = region_tile(d) + lane * half_tiles + j * (chunk // LANES)
        col = pl.multiple_of(tile * LANES, LANES)
        slot = (i % DEPTH) * 4 + q
        if cut is None:
            return pltpu.make_async_copy(table_hbm.at[:, pl.ds(col, chunk)], tbuf.at[slot],
                                         tsem.at[slot // 2])
        lo, hi, sem = cut
        return pltpu.make_async_copy(table_hbm.at[:, pl.ds(col + lo, hi - lo)],
                                     tbuf.at[slot, :, pl.ds(lo, hi - lo)], sem)

    small = [pltpu.make_async_copy(src, dst, in_sem.at[n]) for n, (src, dst) in enumerate(
        ((hid_hbm, hid), (gain_hbm, gain), (tgt_hbm, tgt)))]
    small[0].start()
    small[1].start()
    def first_copy(n):
        q = n % 4
        if n < 4:
            return table_copy(0, q, (0, HEAD, head_sem.at[min(q, 2)]))
        if n < 8:
            return table_copy(0, q, (HEAD, MID, head_sem.at[3 + q // 2]))
        return table_copy(0, q, (MID, chunk, tsem.at[q // 2]))

    for n in (0, 1, 2, 3, 4, 5):
        first_copy(n).start()

    barrier = pltpu.get_barrier_semaphore()
    for peer in (partner, xn, yn):
        pl.semaphore_signal(barrier, inc=1, device_id={'tp': peer}, device_id_type=MESH)

    small[0].wait()
    for n in (6, 7, 8, 9, 10, 11):
        first_copy(n).start()
    h = hid[...].astype(jnp.float32)
    inv_rms = lax.rsqrt(jnp.mean(h * h, axis=-1, keepdims=True) + NORM_EPS)
    small[1].wait()
    gain32[...] = gain[...].astype(jnp.float32)
    g0 = (me * 3) // 2
    hc = hid[:, pl.ds(pl.multiple_of(g0 * LANES, LANES), 2 * LANES)].astype(jnp.float32)
    gc = jnp.concatenate([gain32[pl.ds(g0, 1), :], gain32[pl.ds(g0 + 1, 1), :]], axis=1)

    def own_cols(v):
        return jnp.where(core == 0, v[:, :width], v[:, 2 * LANES - width:])
    normed[...] = (own_cols(hc) * inv_rms * own_cols(gc)).astype(jnp.bfloat16)

    pl.semaphore_wait(barrier, 3)

    def remote(src, dst, kind, recv, device):
        return pltpu.make_async_remote_copy(src_ref=src, dst_ref=dst, send_sem=out_sem.at[kind], recv_sem=recv,
                                            device_id={'tp': device}, device_id_type=MESH)

    def d2d(i, lane):
        return remote(psend.at[i, lane], prec.at[i, lane], 0, d2d_rsem.at[i - (i // (2 * nl)) * (i - 2 * nl)], partner)

    def d2d_part(lane, lo, hi, sem):
        at = pl.ds(lo, hi - lo)
        return remote(psend.at[0, lane, :, at], prec.at[0, lane, :, at], 0, sem, partner)

    def stage1(lane, i):
        return remote(own.at[i, lane], r1.at[i, lane], 1, s1_rsem.at[i // nl], first[lane])

    def stage1_part(lane, lo, hi):
        at = pl.ds(lo, hi - lo)
        return remote(own.at[0, lane, :, at], r1.at[0, lane, :, at], 1, s1_rsem.at[0], first[lane])

    def stage2(lane, j, lo, hi, sem):
        at = pl.ds(lo, hi - lo)
        return remote(own.at[2 * nl + j, lane, :, at], r2.at[j, lane, :, at], 2, s2_rsem.at[sem], second[lane])

    def d2d_pair(i):
        return remote(psend.at[i], prec.at[i], 0, d2d_rsem.at[i], partner)

    def stage2_pair(j, lo, hi, sem):
        at = pl.ds(lo, hi - lo)
        return remote(own.at[2 * nl + j, :, :, at], r2.at[j, :, :, at], 2, s2_rsem.at[sem], yn)

    def multiply(i, q, cols=slice(None)):
        out = psend if q < 2 else own
        slot = (i % DEPTH) * 4 + q
        out[i, q % 2, :, cols] = jnp.dot(normed[...], tbuf[slot, :, cols], preferred_element_type=jnp.float32)

    def pair_wait(i, half):
        slot = (i % DEPTH) * 4 + half * 2
        both = tbuf.at[pl.ds(slot, 2)]
        pltpu.make_async_copy(both, both, tsem.at[slot // 2]).wait()

    def compute(i, qs, prefetch):
        pair_wait(i, qs[0] // 2)
        for q in qs:
            multiply(i, q)
            if q < 2:
                d2d(i, q).start()
            if prefetch is None:
                @pl.when(i + DEPTH < steps)
                def _():
                    table_copy(i + DEPTH, q).start()
            elif prefetch:
                table_copy(i + DEPTH, q).start()

    theirs, ours = (0, 1), (2, 3)

    def piece(half, lo, hi):
        return tbuf.at[pl.ds(2 * half, 2), :, pl.ds(lo, hi - lo)]

    def landed(half, lo, hi, sem):
        pltpu.make_async_copy(piece(half, lo, hi), piece(half, lo, hi), sem).wait()

    def head_pair(lo, hi, sem):
        at = pl.ds(lo, hi - lo)
        remote(psend.at[0, :, :, at], prec.at[0, :, :, at], 0, sem, partner).wait_recv()
        for lane in range(2):
            own[0, lane, :, lo:hi] = own[0, lane, :, lo:hi] + prec[0, lane, :, lo:hi]
            stage1_part(lane, lo, hi).start()

    for q in range(2):
        first_copy(q).wait()
        multiply(0, q, slice(0, HEAD))
        d2d_part(q, 0, HEAD, head_sem.at[5 + q]).start()
    landed(0, HEAD, MID, head_sem.at[3])
    for q in range(2):
        multiply(0, q, slice(HEAD, MID))
        d2d_part(q, HEAD, MID, head_sem.at[7]).start()
    landed(1, 0, HEAD, head_sem.at[2])
    for q in range(2, 4):
        multiply(0, q, slice(0, HEAD))
    for q in range(4):
        table_copy(1, q).start()
    for lane in range(2):
        d2d_part(lane, 0, HEAD, head_sem.at[5 + lane]).wait_recv()
        own[0, lane, :, :HEAD] = own[0, lane, :, :HEAD] + prec[0, lane, :, :HEAD]
        stage1_part(lane, 0, HEAD).start()
    landed(0, MID, chunk, tsem.at[0])
    for q in range(2):
        multiply(0, q, slice(MID, chunk))
        d2d_part(q, MID, chunk, d2d_rsem.at[0]).start()
    landed(1, HEAD, MID, head_sem.at[4])
    for q in range(2, 4):
        multiply(0, q, slice(HEAD, MID))
    head_pair(HEAD, MID, head_sem.at[7])
    for i in range(2, DEPTH):
        for q in range(4):
            table_copy(i, q).start()
    landed(1, MID, chunk, tsem.at[1])
    for q in range(2, 4):
        multiply(0, q, slice(MID, chunk))
    for q in range(4):
        table_copy(DEPTH, q).start()
    small[2].start()
    head_pair(MID, chunk, d2d_rsem.at[0])
    compute(1, theirs, True)
    compute(1, ours, True)
    compute(2, theirs, True)

    def loop_send(i, carry):
        d2d_pair(i).wait_recv()
        for lane in range(2):
            own[i, lane] = own[i, lane] + prec[i, lane]
            stage1(lane, i).start()
        compute(i + 1, ours, True)
        compute(i + 2, theirs, True)
        return carry

    def loop_keep(i, carry):
        compute(i, ours, None)
        compute(i + 1, theirs, None)
        return carry

    lax.fori_loop(1, 2 * nl, loop_send, 0)
    lax.fori_loop(2 * nl + 1, steps - 1, loop_keep, 0)
    compute(steps - 1, ours, False)

    late = pl.ds(2 * nl, 2 * nl)
    remote(psend.at[late], prec.at[late], 0, d2d_rsem.at[2 * nl], partner).wait_recv()
    relay, near = pl.ds(0, nl), pl.ds(nl, nl)
    remote(own.at[relay], r1.at[relay], 1, s1_rsem.at[0], xn).wait_recv()

    pieces = [(j, 0, chunk) for j in range(nl - 1)] + [(nl - 1, 0, chunk - LAST), (nl - 1, chunk - LAST, chunk)]

    def first_sent():
        remote(own.at[pl.ds(0, 2 * nl)], r1, 1, s1_rsem.at[0], xn).wait_send()

    @pl.when(core == 1)
    def _():
        first_sent()

    for n, (j, lo, hi) in enumerate(pieces):
        i = 2 * nl + j
        if n in (1, 2):
            @pl.when(core == 1)
            def _():
                pj, plo, phi = pieces[n - 1]
                stage2_pair(pj, plo, phi, n - 1).wait_send()
        for lane in range(2):
            own[i, lane, :, lo:hi] = own[i, lane, :, lo:hi] + prec[i, lane, :, lo:hi] + r1[j, lane, :, lo:hi]
            stage2(lane, j, lo, hi, n).start()

    remote(own.at[near], r1.at[near], 1, s1_rsem.at[1], xn).wait_recv()

    small[2].wait()
    inv_temp = 1.0 / jnp.full((tokens, LANES), temp[0], jnp.float32)
    row = lax.broadcasted_iota(jnp.int32, (tokens, LANES), 0)
    lane_id = lax.broadcasted_iota(jnp.int32, (tokens, LANES), 1)
    target = jnp.zeros((tokens, LANES), jnp.int32)
    for t in range(tokens):
        target = jnp.where(row == t, tgt[t], target)
    lo_row = me * rows_per
    shift = lo_row - region_tile(me) * LANES
    rel = target - lo_row
    rel = jnp.where((rel >= 0) & (rel < rows_per), rel + shift, -1)
    edge = (0, 1, tiles - 2, tiles - 1)

    m = jnp.full((tokens, LANES), NEG, jnp.float32)
    total = jnp.zeros((tokens, LANES), jnp.float32)
    picked = jnp.zeros((tokens, LANES), jnp.float32)
    for n, (j, lo, hi) in enumerate(pieces):
        i = 3 * nl + j
        stage2_pair(j, lo, hi, n).wait_recv()
        for lane in range(2):
            for at in range(lo, hi, GROUP * LANES):
                parts = []
                top = m
                for k in range(GROUP):
                    c = slice(at + k * LANES, at + (k + 1) * LANES)
                    tile = lane * half_tiles + j * (chunk // LANES) + at // LANES + k
                    z = own[i, lane, :, c] + prec[i, lane, :, c] + r1[nl + j, lane, :, c] + r2[j, lane, :, c]
                    t = z * inv_temp
                    logits[:, tile * LANES:(tile + 1) * LANES] = t
                    picked = picked + jnp.where(lane_id == rel - tile * LANES, t, 0.0)
                    if tile in edge:
                        col = lane_id + (tile * LANES - shift)
                        t = jnp.where((col >= 0) & (col < rows_per), t, NEG)
                    parts.append(t)
                    top = jnp.maximum(top, t)
                total = total * jnp.exp(m - top)
                for t in parts:
                    total = total + jnp.exp(t - top)
                m = top
    m_row = jnp.max(m, axis=-1, keepdims=True)
    s_row = jnp.sum(total * jnp.exp(m - m_row), axis=-1, keepdims=True)
    p_row = jnp.sum(picked, axis=-1, keepdims=True)
    hs = tokens // 2
    lane8 = lax.broadcasted_iota(jnp.int32, (hs, LANES), 1)
    mine[0] = jnp.where(lane8 < 64, jnp.where(lane8 < 32, m_row[:hs], m_row[hs:]),
                        jnp.where(lane8 < 96, p_row[:hs], p_row[hs:]))
    mine[1] = jnp.where(lane8 < 32, s_row[:hs], s_row[hs:])

    def share(peer):
        return remote(mine, every.at[me], 3, st_rsem.at[0], peer)

    far = me + 6 - 4 * mx - 8 * my
    peers = [far, far + 1 - 2 * core, yn, yn + 1 - 2 * core, xn, xn + 1 - 2 * core, partner]
    every[me] = mine[...]
    for peer in peers:
        share(peer).start()

    skip, turn = shift // LANES, shift % LANES
    rot = (LANES - turn) % LANES
    out_tiles = -(-rows_per // LANES)
    keep = lane_id < LANES - turn

    def turned(k):
        at = pl.multiple_of((skip + k) * LANES, LANES)
        return pltpu.roll(logits[:, pl.ds(at, LANES)], rot, axis=1)

    cur = turned(0)
    for k in range(out_tiles):
        if k + 1 < out_tiles:
            nxt = turned(k + 1)
        else:
            nxt = pltpu.roll(logits[:, (tiles - 1) * LANES:tiles * LANES], rot, axis=1)
        shifted[:, k * LANES:(k + 1) * LANES] = jnp.exp(jnp.where(keep, cur, nxt) - m_row)
        cur = nxt

    remote(psend, prec, 0, d2d_rsem.at[0], partner).wait_send()
    @pl.when(core == 0)
    def _():
        first_sent()
    for n, (j, lo, hi) in enumerate(pieces):
        if n + 1 in (1, 2):
            @pl.when(core == 0)
            def _():
                stage2_pair(j, lo, hi, n).wait_send()
        else:
            stage2_pair(j, lo, hi, n).wait_send()

    seven = every.at[pl.ds(0, 7)]
    remote(seven, seven, 3, st_rsem.at[0], partner).wait_recv()
    blocks_ref[...] = every[...]
    remote(seven, seven, 3, st_rsem.at[0], partner).wait_send()


def _finish_kernel(tokens, rows_per, shifted, blocks_ref, probs_hbm, ln_hbm, tl_hbm, probs, ln, tl, sem):
    row = lax.broadcasted_iota(jnp.int32, (tokens, LANES), 0)
    lane_id = lax.broadcasted_iota(jnp.int32, (tokens, LANES), 1)
    def tree(op, vs):
        while len(vs) > 1:
            vs = [op(vs[k], vs[k + 1]) for k in range(0, len(vs), 2)]
        return vs[0]

    def rows16(v, at):
        return jnp.concatenate([v[:, at:at + 1], v[:, at + 32:at + 33]], axis=0)

    tops = [blocks_ref[d, 0] for d in range(8)]
    m_all = tree(jnp.maximum, tops)
    s_all = tree(jnp.add, [blocks_ref[d, 1] * jnp.exp(tops[d] - m_all) for d in range(8)])
    log_all = m_all + jnp.log(s_all)
    scale = rows16(jnp.exp(blocks_ref[lax.axis_index('tp'), 0] - m_all) / s_all, 0)
    log_norm = rows16(log_all, 0)
    p_all = rows16(tree(jnp.add, tops), 64)

    def as_row(v):
        spread = jnp.where(lane_id == row, jnp.broadcast_to(v, (tokens, LANES)), 0.0)
        return jnp.sum(spread, axis=0, keepdims=True)[:, :tokens]

    cut = 76 * LANES
    sides = (pl.ds(0, cut), pl.ds(cut, rows_per - cut))
    copies = [pltpu.make_async_copy(probs.at[:, side], probs_hbm.at[:, side], sem.at[n]) for n, side in enumerate(sides)]
    copies += [pltpu.make_async_copy(ln, ln_hbm, sem.at[2]), pltpu.make_async_copy(tl, tl_hbm, sem.at[3])]
    probs[:, :cut] = (shifted[:, :cut] * scale).astype(jnp.bfloat16)
    copies[0].start()
    ln[...] = as_row(log_norm)
    tl[...] = as_row(p_all - log_norm)
    probs[:, cut:rows_per] = (shifted[:, cut:rows_per] * scale).astype(jnp.bfloat16)
    for c in copies[1:]:
        c.start()
    for c in copies:
        c.wait()


def _scores(hidden, gain, table, targets, temperature):
    tokens, hidden_dim = hidden.shape
    vocab, width = table.shape
    rows_per = vocab // 8
    nl = LANE_CHUNKS
    unit = 2 * nl
    need = -(-rows_per // LANES) + 1
    tiles = -(-need // unit) * unit
    chunk = tiles // unit * LANES
    steps = 4 * nl
    out_tiles = -(-rows_per // LANES)
    f32 = jnp.float32
    dma = pltpu.SemaphoreType.DMA
    block = (tokens, chunk)
    grows = hidden_dim // LANES
    hbm = lambda v: pltpu.with_memory_space_constraint(v, pltpu.HBM)
    shifted, blocks = pl.pallas_call(
        lambda *refs: _kernel((rows_per, tokens, width, tiles, chunk), *refs),
        out_shape=(pltpu.VMEM((tokens, out_tiles * LANES), f32), pltpu.VMEM((8, 2, tokens // 2, LANES), f32)),
        in_specs=[pl.BlockSpec(memory_space=pltpu.HBM)] * 4 + [pl.BlockSpec(memory_space=pltpu.SMEM)],
        out_specs=(pl.BlockSpec(memory_space=pltpu.VMEM),) * 2,
        scratch_shapes=[
            pltpu.VMEM((tokens, hidden_dim), jnp.bfloat16),
            pltpu.VMEM((grows, LANES), jnp.bfloat16),
            pltpu.VMEM((grows, LANES), f32),
            pltpu.SMEM((tokens,), jnp.int32),
            pltpu.VMEM((tokens, width), jnp.bfloat16),
            pltpu.VMEM((DEPTH * 4, width, chunk), jnp.bfloat16),
            pltpu.VMEM((steps, 2) + block, f32),
            pltpu.VMEM((steps, 2) + block, f32),
            pltpu.VMEM((steps, 2) + block, f32),
            pltpu.VMEM((2 * nl, 2) + block, f32),
            pltpu.VMEM((nl, 2) + block, f32),
            pltpu.VMEM((tokens, tiles * LANES), f32),
            pltpu.VMEM((2, tokens // 2, LANES), f32),
            pltpu.VMEM((8, 2, tokens // 2, LANES), f32),
            dma((3,)), dma((DEPTH * 2,)), dma((8,)),
            dma((2 * nl + 1,)), dma((2,)), dma((nl + 1,)), dma((1,)), dma((4,)),
        ],
        compiler_params=pltpu.CompilerParams(collective_id=0, has_side_effects=True,
                                             vmem_limit_bytes=48 * 1024 * 1024),
        name='head',
    )(hbm(hidden), hbm(gain.reshape(grows, LANES)), hbm(table.T), hbm(targets), temperature.reshape(1))
    return pl.pallas_call(
        lambda *refs: _finish_kernel(tokens, rows_per, *refs),
        out_shape=(jax.ShapeDtypeStruct((tokens, rows_per), jnp.bfloat16),
                   jax.ShapeDtypeStruct((1, tokens), f32), jax.ShapeDtypeStruct((1, tokens), f32)),
        in_specs=[pl.BlockSpec(memory_space=pltpu.VMEM)] * 2,
        out_specs=(pl.BlockSpec(memory_space=pltpu.HBM),) * 3,
        scratch_shapes=[pltpu.VMEM((tokens, rows_per), jnp.bfloat16), pltpu.VMEM((1, tokens), f32),
                        pltpu.VMEM((1, tokens), f32), dma((4,))],
        compiler_params=pltpu.CompilerParams(vmem_limit_bytes=16 * 1024 * 1024),
        name='finish',
    )(shifted, blocks)


def solution(mesh):
    def local_scores(hidden, final_gain, table_cols, targets, temperature):
        probs, ln, tl = _scores(hidden, final_gain, table_cols, targets, temperature)
        return ln.reshape(-1), tl.reshape(-1), probs

    return jax.shard_map(local_scores, mesh=mesh,
                         in_specs=(P('dp', None), P(None), P(None, 'tp'), P('dp'), P()),
                         out_specs=(P('dp'), P('dp'), P('dp', 'tp')),
                         check_vma=False)
```

```python
import jax
import jax.numpy as jnp
from jax import lax
from jax.experimental import pallas as pl
from jax.experimental.pallas import tpu as pltpu
from jax.sharding import PartitionSpec as P

NORM_EPS = 1e-6
LANES = 128
LANE_CHUNKS = 3
DEPTH = 2
HEAD, MID = 4 * LANES, 11 * LANES
LAST = 5 * LANES
GROUP = 5
NEG = -3.0e38
MESH = pl.DeviceIdType.MESH


def _kernel(shape, hid_hbm, gain_hbm, table_hbm, tgt_hbm, temp, shifted, blocks_ref,
            hid, gain, gain32, tgt, normed, tbuf, psend, prec, own, r1, r2, logits, mine, every,
            in_sem, tsem, head_sem, d2d_rsem, s1_rsem, s2_rsem, st_rsem, out_sem):
    rows_per, tokens, width, tiles, chunk = shape
    half_tiles = tiles // 2
    nl = LANE_CHUNKS
    steps = 4 * nl
    me = lax.axis_index('tp')
    core, mx, my = me % 2, (me // 2) % 2, me // 4
    partner = me + 1 - 2 * core
    xn = me + 2 - 4 * mx
    yn = me + 4 - 8 * my
    first = (xn, yn)
    second = (yn, xn)

    def region_tile(d):
        return (d * rows_per) // LANES - d // 7

    def table_copy(i, q, cut=None):
        p, j = i // nl, i % nl
        lane = q % 2
        a, b = 1 - p // 2, 1 - p % 2
        fx, fy = (a, b) if lane == 0 else (b, a)
        k = 1 - core if q < 2 else core
        d = (my + fy * (1 - 2 * my)) * 4 + (mx + fx * (1 - 2 * mx)) * 2 + k
        tile = region_tile(d) + lane * half_tiles + j * (chunk // LANES)
        col = pl.multiple_of(tile * LANES, LANES)
        slot = (i % DEPTH) * 4 + q
        if cut is None:
            return pltpu.make_async_copy(table_hbm.at[:, pl.ds(col, chunk)], tbuf.at[slot],
                                         tsem.at[slot // 2])
        lo, hi, sem = cut
        return pltpu.make_async_copy(table_hbm.at[:, pl.ds(col + lo, hi - lo)],
                                     tbuf.at[slot, :, pl.ds(lo, hi - lo)], sem)

    small = [pltpu.make_async_copy(src, dst, in_sem.at[n]) for n, (src, dst) in enumerate(
        ((hid_hbm, hid), (gain_hbm, gain), (tgt_hbm, tgt)))]
    small[0].start()
    small[1].start()
    def first_copy(n):
        q = n % 4
        if n < 4:
            return table_copy(0, q, (0, HEAD, head_sem.at[min(q, 2)]))
        if n < 8:
            return table_copy(0, q, (HEAD, MID, head_sem.at[3 + q // 2]))
        return table_copy(0, q, (MID, chunk, tsem.at[q // 2]))

    for n in (0, 1, 2, 3, 4, 5):
        first_copy(n).start()

    barrier = pltpu.get_barrier_semaphore()
    for peer in (partner, xn, yn):
        pl.semaphore_signal(barrier, inc=1, device_id={'tp': peer}, device_id_type=MESH)

    small[0].wait()
    for n in (6, 7, 8, 9, 10, 11):
        first_copy(n).start()
    h = hid[...].astype(jnp.float32)
    inv_rms = lax.rsqrt(jnp.mean(h * h, axis=-1, keepdims=True) + NORM_EPS)
    small[1].wait()
    gain32[...] = gain[...].astype(jnp.float32)
    g0 = (me * 3) // 2
    hc = hid[:, pl.ds(pl.multiple_of(g0 * LANES, LANES), 2 * LANES)].astype(jnp.float32)
    gc = jnp.concatenate([gain32[pl.ds(g0, 1), :], gain32[pl.ds(g0 + 1, 1), :]], axis=1)

    def own_cols(v):
        return jnp.where(core == 0, v[:, :width], v[:, 2 * LANES - width:])
    normed[...] = (own_cols(hc) * inv_rms * own_cols(gc)).astype(jnp.bfloat16)

    pl.semaphore_wait(barrier, 3)

    def remote(src, dst, kind, recv, device):
        return pltpu.make_async_remote_copy(src_ref=src, dst_ref=dst, send_sem=out_sem.at[kind], recv_sem=recv,
                                            device_id={'tp': device}, device_id_type=MESH)

    def d2d(i, lane):
        return remote(psend.at[i, lane], prec.at[i, lane], 0, d2d_rsem.at[i - (i // (2 * nl)) * (i - 2 * nl)], partner)

    def d2d_part(lane, lo, hi, sem):
        at = pl.ds(lo, hi - lo)
        return remote(psend.at[0, lane, :, at], prec.at[0, lane, :, at], 0, sem, partner)

    def stage1(lane, i):
        return remote(own.at[i, lane], r1.at[i, lane], 1, s1_rsem.at[i // nl], first[lane])

    def stage1_part(lane, lo, hi):
        at = pl.ds(lo, hi - lo)
        return remote(own.at[0, lane, :, at], r1.at[0, lane, :, at], 1, s1_rsem.at[0], first[lane])

    def stage2(lane, j, lo, hi, sem):
        at = pl.ds(lo, hi - lo)
        return remote(own.at[2 * nl + j, lane, :, at], r2.at[j, lane, :, at], 2, s2_rsem.at[sem], second[lane])

    def d2d_pair(i):
        return remote(psend.at[i], prec.at[i], 0, d2d_rsem.at[i], partner)

    def stage2_pair(j, lo, hi, sem):
        at = pl.ds(lo, hi - lo)
        return remote(own.at[2 * nl + j, :, :, at], r2.at[j, :, :, at], 2, s2_rsem.at[sem], yn)

    def multiply(i, q, cols=slice(None)):
        out = psend if q < 2 else own
        slot = (i % DEPTH) * 4 + q
        out[i, q % 2, :, cols] = jnp.dot(normed[...], tbuf[slot, :, cols], preferred_element_type=jnp.float32)

    def pair_wait(i, half):
        slot = (i % DEPTH) * 4 + half * 2
        both = tbuf.at[pl.ds(slot, 2)]
        pltpu.make_async_copy(both, both, tsem.at[slot // 2]).wait()

    def compute(i, qs, prefetch):
        pair_wait(i, qs[0] // 2)
        for q in qs:
            multiply(i, q)
            if q < 2:
                d2d(i, q).start()
            if prefetch is None:
                @pl.when(i + DEPTH < steps)
                def _():
                    table_copy(i + DEPTH, q).start()
            elif prefetch:
                table_copy(i + DEPTH, q).start()

    theirs, ours = (0, 1), (2, 3)

    def piece(half, lo, hi):
        return tbuf.at[pl.ds(2 * half, 2), :, pl.ds(lo, hi - lo)]

    def landed(half, lo, hi, sem):
        pltpu.make_async_copy(piece(half, lo, hi), piece(half, lo, hi), sem).wait()

    def head_pair(lo, hi, sem):
        at = pl.ds(lo, hi - lo)
        remote(psend.at[0, :, :, at], prec.at[0, :, :, at], 0, sem, partner).wait_recv()
        for lane in range(2):
            own[0, lane, :, lo:hi] = own[0, lane, :, lo:hi] + prec[0, lane, :, lo:hi]
            stage1_part(lane, lo, hi).start()

    for q in range(2):
        first_copy(q).wait()
        multiply(0, q, slice(0, HEAD))
        d2d_part(q, 0, HEAD, head_sem.at[5]).start()
    landed(0, HEAD, MID, head_sem.at[3])
    for q in range(2):
        multiply(0, q, slice(HEAD, MID))
        d2d_part(q, HEAD, MID, head_sem.at[6]).start()
    landed(1, 0, HEAD, head_sem.at[2])
    for q in range(2, 4):
        multiply(0, q, slice(0, HEAD))
    for q in range(4):
        table_copy(1, q).start()
    head_pair(0, HEAD, head_sem.at[5])
    landed(0, MID, chunk, tsem.at[0])
    for q in range(2):
        multiply(0, q, slice(MID, chunk))
        d2d_part(q, MID, chunk, d2d_rsem.at[0]).start()
    landed(1, HEAD, MID, head_sem.at[4])
    for q in range(2, 4):
        multiply(0, q, slice(HEAD, MID))
    head_pair(HEAD, MID, head_sem.at[6])
    for i in range(2, DEPTH):
        for q in range(4):
            table_copy(i, q).start()
    landed(1, MID, chunk, tsem.at[1])
    for q in range(2, 4):
        multiply(0, q, slice(MID, chunk))
    for q in range(4):
        table_copy(DEPTH, q).start()
    small[2].start()
    head_pair(MID, chunk, d2d_rsem.at[0])
    compute(1, theirs, True)
    compute(1, ours, True)
    compute(2, theirs, True)

    def loop_send(i, carry):
        d2d_pair(i).wait_recv()
        for lane in range(2):
            own[i, lane] = own[i, lane] + prec[i, lane]
            stage1(lane, i).start()
        compute(i + 1, ours, True)
        compute(i + 2, theirs, True)
        return carry

    def loop_keep(i, carry):
        compute(i, ours, None)
        compute(i + 1, theirs, None)
        return carry

    lax.fori_loop(1, 2 * nl, loop_send, 0)
    lax.fori_loop(2 * nl + 1, steps - 1, loop_keep, 0)
    compute(steps - 1, ours, False)

    late = pl.ds(2 * nl, 2 * nl)
    remote(psend.at[late], prec.at[late], 0, d2d_rsem.at[2 * nl], partner).wait_recv()
    relay, near = pl.ds(0, nl), pl.ds(nl, nl)
    remote(own.at[relay], r1.at[relay], 1, s1_rsem.at[0], xn).wait_recv()

    pieces = [(j, 0, chunk) for j in range(nl - 1)] + [(nl - 1, 0, chunk - LAST), (nl - 1, chunk - LAST, chunk)]

    def first_sent():
        remote(own.at[pl.ds(0, 2 * nl)], r1, 1, s1_rsem.at[0], xn).wait_send()

    @pl.when(core == 1)
    def _():
        first_sent()

    for n, (j, lo, hi) in enumerate(pieces):
        i = 2 * nl + j
        if n in (1, 2):
            @pl.when(core == 1)
            def _():
                pj, plo, phi = pieces[n - 1]
                stage2_pair(pj, plo, phi, n - 1).wait_send()
        for lane in range(2):
            own[i, lane, :, lo:hi] = own[i, lane, :, lo:hi] + prec[i, lane, :, lo:hi] + r1[j, lane, :, lo:hi]
            stage2(lane, j, lo, hi, n).start()

    remote(own.at[near], r1.at[near], 1, s1_rsem.at[1], xn).wait_recv()

    small[2].wait()
    inv_temp = 1.0 / jnp.full((tokens, LANES), temp[0], jnp.float32)
    row = lax.broadcasted_iota(jnp.int32, (tokens, LANES), 0)
    lane_id = lax.broadcasted_iota(jnp.int32, (tokens, LANES), 1)
    target = jnp.zeros((tokens, LANES), jnp.int32)
    for t in range(tokens):
        target = jnp.where(row == t, tgt[t], target)
    lo_row = me * rows_per
    shift = lo_row - region_tile(me) * LANES
    rel = target - lo_row
    rel = jnp.where((rel >= 0) & (rel < rows_per), rel + shift, -1)
    edge = (0, 1, tiles - 2, tiles - 1)

    m = jnp.full((tokens, LANES), NEG, jnp.float32)
    total = jnp.zeros((tokens, LANES), jnp.float32)
    picked = jnp.zeros((tokens, LANES), jnp.float32)
    for n, (j, lo, hi) in enumerate(pieces):
        i = 3 * nl + j
        stage2_pair(j, lo, hi, n).wait_recv()
        for lane in range(2):
            for at in range(lo, hi, GROUP * LANES):
                parts = []
                top = m
                for k in range(GROUP):
                    c = slice(at + k * LANES, at + (k + 1) * LANES)
                    tile = lane * half_tiles + j * (chunk // LANES) + at // LANES + k
                    z = own[i, lane, :, c] + prec[i, lane, :, c] + r1[nl + j, lane, :, c] + r2[j, lane, :, c]
                    t = z * inv_temp
                    logits[:, tile * LANES:(tile + 1) * LANES] = t
                    picked = picked + jnp.where(lane_id == rel - tile * LANES, t, 0.0)
                    if tile in edge:
                        col = lane_id + (tile * LANES - shift)
                        t = jnp.where((col >= 0) & (col < rows_per), t, NEG)
                    parts.append(t)
                    top = jnp.maximum(top, t)
                total = total * jnp.exp(m - top)
                for t in parts:
                    total = total + jnp.exp(t - top)
                m = top
    m_row = jnp.max(m, axis=-1, keepdims=True)
    s_row = jnp.sum(total * jnp.exp(m - m_row), axis=-1, keepdims=True)
    p_row = jnp.sum(picked, axis=-1, keepdims=True)
    hs = tokens // 2
    lane8 = lax.broadcasted_iota(jnp.int32, (hs, LANES), 1)
    mine[0] = jnp.where(lane8 < 64, jnp.where(lane8 < 32, m_row[:hs], m_row[hs:]),
                        jnp.where(lane8 < 96, p_row[:hs], p_row[hs:]))
    mine[1] = jnp.where(lane8 < 32, s_row[:hs], s_row[hs:])

    def share(peer):
        return remote(mine, every.at[me], 3, st_rsem.at[0], peer)

    far = me + 6 - 4 * mx - 8 * my
    peers = [far, far + 1 - 2 * core, yn, yn + 1 - 2 * core, xn, xn + 1 - 2 * core, partner]
    every[me] = mine[...]
    for peer in peers:
        share(peer).start()

    skip, turn = shift // LANES, shift % LANES
    rot = (LANES - turn) % LANES
    out_tiles = -(-rows_per // LANES)
    keep = lane_id < LANES - turn

    def turned(k):
        at = pl.multiple_of((skip + k) * LANES, LANES)
        return pltpu.roll(logits[:, pl.ds(at, LANES)], rot, axis=1)

    cur = turned(0)
    for k in range(out_tiles):
        if k + 1 < out_tiles:
            nxt = turned(k + 1)
        else:
            nxt = pltpu.roll(logits[:, (tiles - 1) * LANES:tiles * LANES], rot, axis=1)
        shifted[:, k * LANES:(k + 1) * LANES] = jnp.exp(jnp.where(keep, cur, nxt) - m_row)
        cur = nxt

    remote(psend, prec, 0, d2d_rsem.at[0], partner).wait_send()
    @pl.when(core == 0)
    def _():
        first_sent()
    for n, (j, lo, hi) in enumerate(pieces):
        if n + 1 in (1, 2):
            @pl.when(core == 0)
            def _():
                stage2_pair(j, lo, hi, n).wait_send()
        else:
            stage2_pair(j, lo, hi, n).wait_send()

    seven = every.at[pl.ds(0, 7)]
    remote(seven, seven, 3, st_rsem.at[0], partner).wait_recv()
    blocks_ref[...] = every[...]
    remote(seven, seven, 3, st_rsem.at[0], partner).wait_send()


def _finish_kernel(tokens, rows_per, shifted, blocks_ref, probs_hbm, ln_hbm, tl_hbm, probs, ln, tl, sem):
    row = lax.broadcasted_iota(jnp.int32, (tokens, LANES), 0)
    lane_id = lax.broadcasted_iota(jnp.int32, (tokens, LANES), 1)
    def tree(op, vs):
        while len(vs) > 1:
            vs = [op(vs[k], vs[k + 1]) for k in range(0, len(vs), 2)]
        return vs[0]

    def rows16(v, at):
        return jnp.concatenate([v[:, at:at + 1], v[:, at + 32:at + 33]], axis=0)

    tops = [blocks_ref[d, 0] for d in range(8)]
    m_all = tree(jnp.maximum, tops)
    s_all = tree(jnp.add, [blocks_ref[d, 1] * jnp.exp(tops[d] - m_all) for d in range(8)])
    log_all = m_all + jnp.log(s_all)
    scale = rows16(jnp.exp(blocks_ref[lax.axis_index('tp'), 0] - m_all) / s_all, 0)
    log_norm = rows16(log_all, 0)
    p_all = rows16(tree(jnp.add, tops), 64)

    def as_row(v):
        spread = jnp.where(lane_id == row, jnp.broadcast_to(v, (tokens, LANES)), 0.0)
        return jnp.sum(spread, axis=0, keepdims=True)[:, :tokens]

    cut = 76 * LANES
    sides = (pl.ds(0, cut), pl.ds(cut, rows_per - cut))
    copies = [pltpu.make_async_copy(probs.at[:, side], probs_hbm.at[:, side], sem.at[n]) for n, side in enumerate(sides)]
    copies += [pltpu.make_async_copy(ln, ln_hbm, sem.at[2]), pltpu.make_async_copy(tl, tl_hbm, sem.at[3])]
    probs[:, :cut] = (shifted[:, :cut] * scale).astype(jnp.bfloat16)
    copies[0].start()
    ln[...] = as_row(log_norm)
    tl[...] = as_row(p_all - log_norm)
    probs[:, cut:rows_per] = (shifted[:, cut:rows_per] * scale).astype(jnp.bfloat16)
    for c in copies[1:]:
        c.start()
    for c in copies:
        c.wait()


def _scores(hidden, gain, table, targets, temperature):
    tokens, hidden_dim = hidden.shape
    vocab, width = table.shape
    rows_per = vocab // 8
    nl = LANE_CHUNKS
    unit = 2 * nl
    need = -(-rows_per // LANES) + 1
    tiles = -(-need // unit) * unit
    chunk = tiles // unit * LANES
    steps = 4 * nl
    out_tiles = -(-rows_per // LANES)
    f32 = jnp.float32
    dma = pltpu.SemaphoreType.DMA
    block = (tokens, chunk)
    grows = hidden_dim // LANES
    hbm = lambda v: pltpu.with_memory_space_constraint(v, pltpu.HBM)
    shifted, blocks = pl.pallas_call(
        lambda *refs: _kernel((rows_per, tokens, width, tiles, chunk), *refs),
        out_shape=(pltpu.VMEM((tokens, out_tiles * LANES), f32), pltpu.VMEM((8, 2, tokens // 2, LANES), f32)),
        in_specs=[pl.BlockSpec(memory_space=pltpu.HBM)] * 4 + [pl.BlockSpec(memory_space=pltpu.SMEM)],
        out_specs=(pl.BlockSpec(memory_space=pltpu.VMEM),) * 2,
        scratch_shapes=[
            pltpu.VMEM((tokens, hidden_dim), jnp.bfloat16),
            pltpu.VMEM((grows, LANES), jnp.bfloat16),
            pltpu.VMEM((grows, LANES), f32),
            pltpu.SMEM((tokens,), jnp.int32),
            pltpu.VMEM((tokens, width), jnp.bfloat16),
            pltpu.VMEM((DEPTH * 4, width, chunk), jnp.bfloat16),
            pltpu.VMEM((steps, 2) + block, f32),
            pltpu.VMEM((steps, 2) + block, f32),
            pltpu.VMEM((steps, 2) + block, f32),
            pltpu.VMEM((2 * nl, 2) + block, f32),
            pltpu.VMEM((nl, 2) + block, f32),
            pltpu.VMEM((tokens, tiles * LANES), f32),
            pltpu.VMEM((2, tokens // 2, LANES), f32),
            pltpu.VMEM((8, 2, tokens // 2, LANES), f32),
            dma((3,)), dma((DEPTH * 2,)), dma((7,)),
            dma((2 * nl + 1,)), dma((2,)), dma((nl + 1,)), dma((1,)), dma((4,)),
        ],
        compiler_params=pltpu.CompilerParams(collective_id=0, has_side_effects=True,
                                             vmem_limit_bytes=48 * 1024 * 1024),
        name='head',
    )(hbm(hidden), hbm(gain.reshape(grows, LANES)), hbm(table.T), hbm(targets), temperature.reshape(1))
    return pl.pallas_call(
        lambda *refs: _finish_kernel(tokens, rows_per, *refs),
        out_shape=(jax.ShapeDtypeStruct((tokens, rows_per), jnp.bfloat16),
                   jax.ShapeDtypeStruct((1, tokens), f32), jax.ShapeDtypeStruct((1, tokens), f32)),
        in_specs=[pl.BlockSpec(memory_space=pltpu.VMEM)] * 2,
        out_specs=(pl.BlockSpec(memory_space=pltpu.HBM),) * 3,
        scratch_shapes=[pltpu.VMEM((tokens, rows_per), jnp.bfloat16), pltpu.VMEM((1, tokens), f32),
                        pltpu.VMEM((1, tokens), f32), dma((4,))],
        compiler_params=pltpu.CompilerParams(vmem_limit_bytes=16 * 1024 * 1024),
        name='finish',
    )(shifted, blocks)


def solution(mesh):
    def local_scores(hidden, final_gain, table_cols, targets, temperature):
        probs, ln, tl = _scores(hidden, final_gain, table_cols, targets, temperature)
        return ln.reshape(-1), tl.reshape(-1), probs

    return jax.shard_map(local_scores, mesh=mesh,
                         in_specs=(P('dp', None), P(None), P(None, 'tp'), P('dp'), P()),
                         out_specs=(P('dp'), P('dp'), P('dp', 'tp')),
                         check_vma=False)
```
